256 devices in a mesh: row: 8 (over x, core), col: 32 (over z, y).
Axes of the slice: x: 4, y: 4, z: 8, core: 2. Of those that a mesh axis runs over, the one named last changes fastest.
Arguments:
- momentum: bfloat16 [8192, 32768], P('row', 'col'), may hold values from -240 to 240
- gradient: bfloat16 [8192, 32768], P('row', 'col'), may hold values from -6 to 6
- right_basis: float32 [32768, 256], P('col'), may hold values from -0.03125 to 0.03125
Outputs:
- new_momentum: bfloat16 [8192, 32768], P('row', 'col')
- new_basis: float32 [32768, 256], P('col')
- update: float32 [8192, 32768], P('row', 'col')
The draws below stay inside these ranges and needn't reach their ends.
All inputs are finite; a program needn't handle non-finite values.
Results may differ from the reference program's by a relative error of at most 0.001.
Values sent between devices are 32-bit elements; how exact they have to be, the bound alone decides.
No kernel may reach another device: no remote copies, remote signals or barrier semaphores. Data moves between devices by JAX's collectives and lax.ppermute only.
A program may use at most 64 MiB of HBM per device.

```python
import math
import jax
import jax.numpy as jnp
from jax import lax

ROWS = 8192
COLS = 32768
RANK = 256


def draw_momentum(key, part):
    keys = jax.random.split(jax.random.fold_in(key, 7), 3)
    noise = jax.random.truncated_normal(keys[0], -4.0, 4.0, (ROWS, COLS), jnp.float32)
    row_scales = jnp.exp(jax.random.uniform(keys[1], (ROWS, 1), jnp.float32, math.log(0.3), math.log(3.0)))
    rising = 3.0 ** (jnp.arange(COLS, dtype=jnp.float32) / COLS)
    col_scales = jnp.exp(jax.random.uniform(keys[2], (1, COLS), jnp.float32, math.log(0.2), math.log(2.0))) * rising[None, :]
    return (noise * row_scales * col_scales).astype(jnp.bfloat16)


def block_scale(rng, dims, cuts, smallest, high):
    loudness, own = 1.0, jax.random.fold_in(rng, 6)
    for position, shards_of in cuts:
        draws = jnp.exp(jax.random.uniform(jax.random.fold_in(own, position), (shards_of,), jnp.float32, smallest / len(cuts), high / len(cuts)))
        loudness = loudness * jnp.repeat(draws, dims[position] // shards_of).reshape([-1 if axis == position else 1 for axis in range(len(dims))])
    return loudness


def centred(stream_key, extent, width, bound, cuts=(), held_as=jnp.bfloat16):
    gain = block_scale(stream_key, extent, cuts, -0.22, 0.18) if cuts else 1.0
    result = jax.random.normal(stream_key, extent, jnp.float32) * width * gain
    return jnp.minimum(jnp.maximum(result, -bound), bound).astype(held_as)


def setup_inputs(seed: int = 0) -> dict:
    arg_keys = jax.random.split(jax.random.key(seed), 4)
    momentum = draw_momentum(jax.random.fold_in(arg_keys[3], 71), 0)
    gradient = centred(arg_keys[1], (ROWS, COLS), 1.0, 6.0, ((0, 8), (1, 32)))
    right_basis = centred(arg_keys[2], (COLS, RANK), COLS ** -0.5, 0.03125, ((0, 32),), jnp.float32)
    return dict(momentum=momentum, gradient=gradient, right_basis=right_basis)


eps = 1e-08
momentum_decay = 0.95

def reference(momentum, gradient, right_basis):
    highest = lax.Precision.HIGHEST
    summed = momentum.astype(jnp.float32) + gradient.astype(jnp.float32)
    projected = jnp.dot(summed, right_basis, precision=highest)
    gram_matrix = jnp.dot(projected.T, projected, precision=highest)
    factor = jnp.linalg.cholesky(gram_matrix)
    orthonormal = jax.scipy.linalg.solve_triangular(factor, projected.T, lower=True).T
    flipped = jnp.dot(orthonormal.T, summed, precision=highest)
    squares = lax.optimization_barrier(jnp.sum(flipped * flipped, axis=1))
    normed = flipped / (jnp.sqrt(squares)[:, None] + eps)
    new_momentum = (summed - (1.0 - momentum_decay) * jnp.dot(orthonormal, flipped, precision=highest)).astype(jnp.bfloat16)
    rms_scale = math.sqrt(ROWS * COLS / RANK)
    update = rms_scale * jnp.dot(orthonormal, normed, precision=highest)
    return (new_momentum, normed.T, update)
```

```python
import math

import jax
import jax.numpy as jnp
from jax import lax
from jax.sharding import Mesh
from jax.sharding import PartitionSpec as P

ROWS = 8192
COLS = 32768
RANK = 256
COL = ("z", "y")
ROW = ("x", "c")


eps = 1e-08
momentum_decay = 0.95


def scattered(array, axis):
    tiles = array.reshape(lax.axis_size(axis), -1, array.shape[-1])
    return lax.all_to_all(tiles, axis, 0, 0, tiled=True).sum(axis=0)


def from_everyone(array, axis):
    tiles = jnp.broadcast_to(array[None], (lax.axis_size(axis), *array.shape))
    return lax.all_to_all(tiles, axis, 0, 0, tiled=True)


def gathered(array, axis):
    return from_everyone(array, axis).reshape(-1, array.shape[-1])


def other_core(array):
    return lax.ppermute(array, "c", [(0, 1), (1, 0)])


def dot(left, right, left_dim, right_dim, precision):
    return lax.dot_general(
        left,
        right,
        (((left_dim,), (right_dim,)), ((), ())),
        precision=precision,
        preferred_element_type=jnp.float32,
    )


def in_core_order(core, own, other, dim=0):
    first = jnp.where(core == 0, own, other)
    second = jnp.where(core == 0, other, own)
    return jnp.concatenate((first, second), axis=dim)


def shards(momentum, gradient, right_basis):
    high, highest = lax.Precision.HIGH, lax.Precision.HIGHEST
    core = lax.axis_index("c")
    summed = momentum.astype(jnp.float32) + gradient.astype(jnp.float32)

    part = dot(summed, right_basis, 1, 0, high)
    own = scattered(scattered(part, "y"), "z")
    projected = gathered(gathered(own, "z"), "y")

    gram = dot(projected, projected, 0, 0, highest)
    wide = dot(summed, projected, 0, 0, high)
    halves = wide.reshape(2, -1, RANK)
    kept = lax.dynamic_index_in_dim(halves, core, 0, keepdims=False)
    given = lax.dynamic_index_in_dim(halves, 1 - core, 0, keepdims=False)
    wide_half = kept + other_core(given)
    gram = gram + other_core(gram)
    gram_half = lax.dynamic_slice_in_dim(gram, core * (RANK // 2), RANK // 2, 0)
    sides = lax.axis_size("x")
    tiles = jnp.concatenate(
        (
            wide_half.reshape(sides, -1, RANK),
            jnp.broadcast_to(gram_half[None], (sides, *gram_half.shape)),
        ),
        axis=1,
    )
    arrived = lax.all_to_all(tiles, "x", 0, 0, tiled=True).sum(axis=0)
    wide_own, gram_half = arrived[: -RANK // 2], arrived[-RANK // 2 :]
    gram_matrix = in_core_order(core, gram_half, other_core(gram_half))
    wide_half = gathered(wide_own, "x")
    wide = in_core_order(core, wide_half, other_core(wide_half))

    factor = jnp.linalg.cholesky(gram_matrix)
    inverse = jax.scipy.linalg.solve_triangular(
        factor, jnp.eye(RANK, dtype=jnp.float32), lower=True
    )
    orthonormal = dot(projected, inverse, 1, 1, highest)
    transposed = dot(wide, inverse, 1, 1, highest)

    squares = from_everyone(jnp.sum(transposed * transposed, axis=0)[None], COL).sum(axis=0)
    new_momentum = (
        summed - dot((1.0 - momentum_decay) * orthonormal, transposed, 1, 1, high)
    ).astype(jnp.bfloat16)
    new_basis = transposed / (jnp.sqrt(squares) + eps)
    rms_scale = math.sqrt(ROWS * COLS / RANK)
    update = dot(rms_scale * orthonormal, new_basis, 1, 1, high)
    return (new_momentum, new_basis, update)


def solution(mesh):
    split = Mesh(mesh.devices.reshape(4, 2, 8, 4), (*ROW, *COL))
    placed = (P(ROW, COL), P(ROW, COL), P(COL, None))
    return jax.shard_map(
        shards,
        mesh=split,
        in_specs=placed,
        out_specs=(P(ROW, COL), P(COL, None), P(ROW, COL)),
        check_vma=False,
    )
```

```python
import math

import jax
import jax.numpy as jnp
from jax import lax
from jax.experimental import pallas as pl
from jax.experimental.pallas import tpu as pltpu
from jax.sharding import Mesh
from jax.sharding import PartitionSpec as P

ROWS = 8192
COLS = 32768
RANK = 256
COL = ("z", "y")
ROW = ("x", "c")


eps = 1e-08
momentum_decay = 0.95


def scattered(array, axis):
    tiles = array.reshape(lax.axis_size(axis), -1, array.shape[-1])
    return lax.all_to_all(tiles, axis, 0, 0, tiled=True).sum(axis=0)


def from_everyone(array, axis):
    tiles = jnp.broadcast_to(array[None], (lax.axis_size(axis), *array.shape))
    return lax.all_to_all(tiles, axis, 0, 0, tiled=True)


def gathered(array, axis):
    return from_everyone(array, axis).reshape(-1, array.shape[-1])


def other_core(array):
    return lax.ppermute(array, "c", [(0, 1), (1, 0)])


def dot(left, right, left_dim, right_dim, precision):
    return lax.dot_general(
        left,
        right,
        (((left_dim,), (right_dim,)), ((), ())),
        precision=precision,
        preferred_element_type=jnp.float32,
    )


def in_core_order(core, own, other, dim=0):
    first = jnp.where(core == 0, own, other)
    second = jnp.where(core == 0, other, own)
    return jnp.concatenate((first, second), axis=dim)


def mxu(left, right, dims):
    return lax.dot_general(left, right, (dims, ((), ())), preferred_element_type=jnp.float32)

def parts(array):
    top = array.astype(jnp.bfloat16)
    return top, (array - top.astype(jnp.float32)).astype(jnp.bfloat16)

def dot3(left, right, dims):
    (a, b), (c, d) = parts(left), parts(right)
    return mxu(a, c, dims) + (mxu(a, d, dims) + mxu(b, c, dims))

def dot1(left, right, dims):
    return mxu(left.astype(jnp.bfloat16), right.astype(jnp.bfloat16), dims)

PLAIN = ((1,), (0,))
FLIPPED = ((1,), (1,))

def inverse_factor(gram_ref, out_ref, work):
    shape = (RANK, RANK)
    row, column = (lax.broadcasted_iota(jnp.int32, shape, d) for d in (0, 1))
    eye = (row == column).astype(jnp.float32)
    lower = jnp.where(row > column, 1.0, 0.5 * eye)
    gram = gram_ref[...]
    diagonal = gram * eye
    along = lax.rsqrt(jnp.sum(diagonal, axis=0, keepdims=True))
    down = lax.rsqrt(jnp.sum(diagonal, axis=1, keepdims=True))
    scaled = gram * down * along

    def step(guess, dot):
        error = dot(dot(guess, scaled, PLAIN), guess, FLIPPED) - eye
        return guess - dot1(error * lower, guess, PLAIN), error

    guess = eye - (scaled - eye) * lower
    guess, _ = step(guess, dot1)
    guess, _ = step(guess, dot3)
    guess, error = step(guess, dot3)
    out_ref[...] = guess * along

    @pl.when(jnp.logical_not(jnp.sum(error * error) < 1e-4))
    def _():
        work[:, :RANK] = gram
        work[:, RANK:] = eye
        rows = lax.broadcasted_iota(jnp.int32, (RANK, 1), 0)
        lanes = lax.broadcasted_iota(jnp.int32, (1, RANK), 1)

        def eliminate(i, carry):
            line = work[pl.ds(i, 1), :]
            pivot = jnp.sum(jnp.where(lanes == i, line[:, :RANK], 0.0), axis=1, keepdims=True)
            root = lax.rsqrt(pivot)
            line = line * root
            whole = work[...]
            beneath = jnp.sum(jnp.where(lanes == i, whole[:, :RANK], 0.0), axis=1, keepdims=True) * root
            rest = whole - jnp.where(rows > i, beneath, 0.0) * line
            work[...] = jnp.where(rows == i, line, rest)
            return carry

        lax.fori_loop(0, RANK, eliminate, 0)
        out_ref[...] = jnp.where(row >= column, work[:, RANK:], 0.0)

def inverted(gram):
    return pl.pallas_call(
        inverse_factor,
        out_shape=jax.ShapeDtypeStruct((RANK, RANK), jnp.float32),
        scratch_shapes=[pltpu.VMEM((RANK, 2 * RANK), jnp.float32)],
        cost_estimate=pl.CostEstimate(flops=2*9*3*RANK**3, bytes_accessed=8*RANK**2, transcendentals=0),
        name="inverse_factor",
    )(gram)


def shards(momentum, gradient, right_basis):
    high, highest = lax.Precision.HIGH, lax.Precision.HIGHEST
    core = lax.axis_index("c")
    summed = momentum.astype(jnp.float32) + gradient.astype(jnp.float32)

    part = dot(summed, right_basis, 1, 0, high)
    own = scattered(scattered(part, "y"), "z")
    projected = gathered(gathered(own, "z"), "y")

    gram = dot(projected, projected, 0, 0, highest)
    wide = dot(summed, projected, 0, 0, high)
    halves = wide.reshape(2, -1, RANK)
    kept = lax.dynamic_index_in_dim(halves, core, 0, keepdims=False)
    given = lax.dynamic_index_in_dim(halves, 1 - core, 0, keepdims=False)
    wide_half = kept + other_core(given)
    gram = gram + other_core(gram)
    gram_half = lax.dynamic_slice_in_dim(gram, core * (RANK // 2), RANK // 2, 0)
    sides = lax.axis_size("x")
    tiles = jnp.concatenate(
        (
            wide_half.reshape(sides, -1, RANK),
            jnp.broadcast_to(gram_half[None], (sides, *gram_half.shape)),
        ),
        axis=1,
    )
    arrived = lax.all_to_all(tiles, "x", 0, 0, tiled=True).sum(axis=0)
    wide_own, gram_half = arrived[: -RANK // 2], arrived[-RANK // 2 :]
    gram_matrix = in_core_order(core, gram_half, other_core(gram_half))
    wide_half = gathered(wide_own, "x")
    wide = in_core_order(core, wide_half, other_core(wide_half))

    inverse = inverted(gram_matrix)
    orthonormal = dot(projected, inverse, 1, 1, highest)
    transposed = dot(wide, inverse, 1, 1, highest)

    squares = from_everyone(jnp.sum(transposed * transposed, axis=0)[None], COL).sum(axis=0)
    new_momentum = (
        summed - dot((1.0 - momentum_decay) * orthonormal, transposed, 1, 1, high)
    ).astype(jnp.bfloat16)
    new_basis = transposed / (jnp.sqrt(squares) + eps)
    rms_scale = math.sqrt(ROWS * COLS / RANK)
    update = dot(rms_scale * orthonormal, new_basis, 1, 1, high)
    return (new_momentum, new_basis, update)


def solution(mesh):
    split = Mesh(mesh.devices.reshape(4, 2, 8, 4), (*ROW, *COL))
    placed = (P(ROW, COL), P(ROW, COL), P(COL, None))
    return jax.shard_map(
        shards,
        mesh=split,
        in_specs=placed,
        out_specs=(P(ROW, COL), P(COL, None), P(ROW, COL)),
        check_vma=False,
    )
```

```python
import math

import jax
import jax.numpy as jnp
from jax import lax
from jax.experimental import pallas as pl
from jax.experimental.pallas import tpu as pltpu
from jax.sharding import Mesh
from jax.sharding import PartitionSpec as P

ROWS = 8192
COLS = 32768
RANK = 256
COL = ("z", "y")
ROW = ("x", "c")


eps = 1e-08
momentum_decay = 0.95


def scattered(array, axis):
    tiles = array.reshape(lax.axis_size(axis), -1, array.shape[-1])
    return lax.all_to_all(tiles, axis, 0, 0, tiled=True).sum(axis=0)


def from_everyone(array, axis):
    tiles = jnp.broadcast_to(array[None], (lax.axis_size(axis), *array.shape))
    return lax.all_to_all(tiles, axis, 0, 0, tiled=True)


def gathered(array, axis):
    return from_everyone(array, axis).reshape(-1, array.shape[-1])


def other_core(array):
    return lax.ppermute(array, "c", [(0, 1), (1, 0)])


def mxu(left, right, dims):
    return lax.dot_general(left, right, (dims, ((), ())), preferred_element_type=jnp.float32)

def parts(array):
    top = array.astype(jnp.bfloat16)
    return top, (array - top.astype(jnp.float32)).astype(jnp.bfloat16)

def dot3(left, right, dims):
    (a, b), (c, d) = parts(left), parts(right)
    return mxu(a, c, dims) + (mxu(a, d, dims) + mxu(b, c, dims))

def dot1(left, right, dims):
    return mxu(left.astype(jnp.bfloat16), right.astype(jnp.bfloat16), dims)

PLAIN = ((1,), (0,))
FLIPPED = ((1,), (1,))

def core_number():
    return lax.axis_index("c").astype(jnp.int32)[None]


def cost(flops):
    return pl.CostEstimate(flops=flops, bytes_accessed=0, transcendentals=0)


IN_VMEM = pl.BlockSpec(memory_space=pltpu.VMEM)
IN_SMEM = pl.BlockSpec(memory_space=pltpu.SMEM)
TILE = 256
HALF = RANK // 2
PACKED = 3 * HALF // 4


def wider(tile):
    return tile.astype(jnp.float32)


def split_dot(left, right, dims):
    (a, b), (c, d) = left, right
    return mxu(a, c, dims) + (mxu(a, d, dims) + mxu(b, c, dims))


def limit(mib):
    return pltpu.CompilerParams(vmem_limit_bytes=mib << 20)


def project_kernel(momentum, gradient, basis, out, top, low):
    a, b = parts(wider(momentum[...]) + wider(gradient[...]))
    top[...], low[...] = a, b
    right = parts(basis[...])
    rows = out.shape[0]

    @pl.when(pl.program_id(0) == 0)
    def _():
        out[...] = split_dot((a, b), right, PLAIN)

    @pl.when(pl.program_id(0) > 0)
    def _():
        out[...] += split_dot((a, b), right, PLAIN)


def project(momentum, gradient, basis):
    rows, columns = momentum.shape
    block = pl.BlockSpec((rows, TILE), lambda t: (0, t))
    split = jax.ShapeDtypeStruct((rows, columns), jnp.bfloat16)
    return pl.pallas_call(
        project_kernel,
        grid=(columns // TILE,),
        in_specs=[block, block, pl.BlockSpec((TILE, RANK), lambda t: (t, 0))],
        out_specs=[pl.BlockSpec((rows, RANK), lambda t: (0, 0)), block, block],
        out_shape=[jax.ShapeDtypeStruct((rows, RANK), jnp.float32), split, split],
        cost_estimate=cost(6 * rows * columns * RANK),
        compiler_params=limit(61),
        name="project",
    )(momentum, gradient, basis)


def widen_kernel(core, top, low, projected, outgoing, kept, flat_top, flat_low):
    half = kept.shape[0]
    across = parts(projected[...].T)
    flat_top[...], flat_low[...] = across

    for place, target in ((1 - core[0], outgoing), (core[0], kept)):

        @pl.loop(0, half // TILE)
        def _(t):
            span = pl.ds(pl.multiple_of(place * half + t * TILE, TILE), TILE)
            tile = split_dot(
                (flat_top[...], flat_low[...]), (top[:, span], low[:, span]), PLAIN
            )
            target[pl.ds(pl.multiple_of(t * TILE, TILE), TILE), :] = tile.T

    outgoing[half:, :] = split_dot(
        (flat_top[...], flat_low[...]), parts(projected[...]), PLAIN
    )


def widen(core, top, low, projected):
    rows, columns = top.shape
    return pl.pallas_call(
        widen_kernel,
        in_specs=[IN_SMEM, IN_VMEM, IN_VMEM, IN_VMEM],
        out_specs=[IN_VMEM, IN_VMEM],
        out_shape=[
            jax.ShapeDtypeStruct((columns // 2 + RANK, RANK), jnp.float32),
            jax.ShapeDtypeStruct((columns // 2, RANK), jnp.float32),
        ],
        scratch_shapes=[pltpu.VMEM((RANK, rows), jnp.bfloat16)] * 2,
        cost_estimate=cost(6 * rows * (columns + RANK) * RANK),
        compiler_params=limit(20),
        name="widen",
    )(core, top, low, projected)


def folded(block):
    half = block.shape[0] // 2
    return jnp.concatenate((block[:half], block[half:]), axis=1)


def unfolded(block):
    return jnp.concatenate((block[:, :HALF], block[:, HALF:]), axis=0)


def merge_kernel(core, outgoing, received, kept, out):
    sides = out.shape[0]
    each = kept.shape[0] // sides
    for side in range(sides):
        span = pl.ds(side * each, each)
        out[side, :each, :] = kept[span, :] + received[span, :]
    gram = outgoing[kept.shape[0] :, :] + received[kept.shape[0] :, :]
    corner = gram[HALF:, :HALF]

    def put(square, strip):
        for side in range(sides):
            out[side, each : each + HALF // 2, :] = folded(square)
            out[side, each + HALF // 2 :, :] = folded(strip)

    @pl.when(core[0] == 0)
    def _():
        put(gram[:HALF, :HALF], corner[: HALF // 2])

    @pl.when(core[0] == 1)
    def _():
        put(gram[HALF:, HALF:], corner[HALF // 2 :])


def merge(core, outgoing, received, kept, sides):
    each = kept.shape[0] // sides
    return pl.pallas_call(
        merge_kernel,
        in_specs=[IN_SMEM, IN_VMEM, IN_VMEM, IN_VMEM],
        out_specs=IN_VMEM,
        out_shape=jax.ShapeDtypeStruct((sides, each + PACKED, RANK), jnp.float32),
        cost_estimate=cost(kept.size),
        compiler_params=pltpu.CompilerParams(vmem_limit_bytes=8 << 20),
        name="merge",
    )(core, outgoing, received, kept)


def spread_kernel(arrived, tiles, gram_half):
    sides, each, _ = tiles.shape
    wide = arrived[0, :each, :]
    gram = arrived[0, each:, :]
    for side in range(1, sides):
        wide = wide + arrived[side, :each, :]
        gram = gram + arrived[side, each:, :]
    for side in range(sides):
        tiles[side] = wide
    gram_half[...] = gram


def spread(arrived):
    sides, lines, _ = arrived.shape
    return pl.pallas_call(
        spread_kernel,
        in_specs=[IN_VMEM],
        out_specs=[IN_VMEM, IN_VMEM],
        out_shape=[
            jax.ShapeDtypeStruct((sides, lines - PACKED, RANK), jnp.float32),
            jax.ShapeDtypeStruct((PACKED, RANK), jnp.float32),
        ],
        cost_estimate=cost(arrived.size),
        compiler_params=limit(6),
        name="spread",
    )(arrived)


def inverse_factor(core, own, other, projected, out_ref, orthonormal, work):
    first = jnp.where(core[0] == 0, own[...], other[...])
    second = jnp.where(core[0] == 0, other[...], own[...])
    corner = jnp.concatenate((unfolded(first[HALF // 2 :]), unfolded(second[HALF // 2 :])), axis=0)
    gram = jnp.concatenate(
        (
            jnp.concatenate((unfolded(first[: HALF // 2]), corner.T), axis=1),
            jnp.concatenate((corner, unfolded(second[: HALF // 2])), axis=1),
        ),
        axis=0,
    )
    shape = (RANK, RANK)
    row, column = (lax.broadcasted_iota(jnp.int32, shape, d) for d in (0, 1))
    eye = (row == column).astype(jnp.float32)
    lower = jnp.where(row > column, 1.0, 0.5 * eye)
    diagonal = gram * eye
    along = lax.rsqrt(jnp.sum(diagonal, axis=0, keepdims=True))
    down = lax.rsqrt(jnp.sum(diagonal, axis=1, keepdims=True))
    scaled = gram * down * along

    def step(guess, dot):
        error = dot(dot(guess, scaled, PLAIN), guess, FLIPPED) - eye
        return guess - dot1(error * lower, guess, PLAIN), error

    guess = eye - (scaled - eye) * lower
    guess, _ = step(guess, dot1)
    guess, _ = step(guess, dot3)
    guess, error = step(guess, dot3)
    out_ref[...] = guess * along

    @pl.when(jnp.logical_not(jnp.sum(error * error) < 1e-4))
    def _():
        work[:, :RANK] = gram
        work[:, RANK:] = eye
        rows = lax.broadcasted_iota(jnp.int32, (RANK, 1), 0)
        lanes = lax.broadcasted_iota(jnp.int32, (1, RANK), 1)

        def eliminate(i, carry):
            line = work[pl.ds(i, 1), :]
            pivot = jnp.sum(jnp.where(lanes == i, line[:, :RANK], 0.0), axis=1, keepdims=True)
            root = lax.rsqrt(pivot)
            line = line * root
            whole = work[...]
            beneath = jnp.sum(jnp.where(lanes == i, whole[:, :RANK], 0.0), axis=1, keepdims=True) * root
            rest = whole - jnp.where(rows > i, beneath, 0.0) * line
            work[...] = jnp.where(rows == i, line, rest)
            return carry

        lax.fori_loop(0, RANK, eliminate, 0)
        out_ref[...] = jnp.where(row >= column, work[:, RANK:], 0.0)

    right = parts(out_ref[...])

    @pl.loop(0, projected.shape[0] // TILE)
    def _(t):
        span = pl.ds(pl.multiple_of(t * TILE, TILE), TILE)
        orthonormal[span, :] = split_dot(parts(projected[span, :]), right, FLIPPED)


def inverted(core, own, other, projected):
    return pl.pallas_call(
        inverse_factor,
        in_specs=[IN_SMEM, IN_VMEM, IN_VMEM, IN_VMEM],
        out_specs=[IN_VMEM, IN_VMEM],
        out_shape=[
            jax.ShapeDtypeStruct((RANK, RANK), jnp.float32),
            jax.ShapeDtypeStruct(projected.shape, jnp.float32),
        ],
        scratch_shapes=[pltpu.VMEM((RANK, 2 * RANK), jnp.float32)],
        cost_estimate=cost(1 << 32),
        compiler_params=limit(12),
        name="inverse_factor",
    )(core, own, other, projected)


def transposed_kernel(wide, inverse, out, squares):
    c, d = parts(inverse[...])
    total = jnp.zeros((1, RANK), jnp.float32)
    for t in range(wide.shape[0] // TILE):
        span = slice(t * TILE, (t + 1) * TILE)
        a, b = parts(wide[span, :])
        tile = mxu(a, c, FLIPPED) + (mxu(a, d, FLIPPED) + mxu(b, c, FLIPPED))
        out[span, :] = tile
        total += jnp.sum(tile * tile, axis=0, keepdims=True)
    squares[...] = jnp.broadcast_to(total[None], squares.shape)


def transpose_of(wide, inverse, copies):
    return pl.pallas_call(
        transposed_kernel,
        in_specs=[IN_VMEM, IN_VMEM],
        out_specs=[IN_VMEM, IN_VMEM],
        out_shape=[
            jax.ShapeDtypeStruct(wide.shape, jnp.float32),
            jax.ShapeDtypeStruct((copies, 1, RANK), jnp.float32),
        ],
        cost_estimate=cost(6 * wide.size * RANK),
        compiler_params=pltpu.CompilerParams(vmem_limit_bytes=8 << 20),
        name="transposed",
    )(wide, inverse)


SPAN = 512


def momentum_kernel(core, momentum, gradient, orthonormal, own, other, out, top, low):
    @pl.when(pl.program_id(1) == 0)
    def _():
        top[...], low[...] = parts(jnp.where(pl.program_id(0) == 0, own[...], other[...]))

    left = parts((1.0 - momentum_decay) * orthonormal[...])
    product = split_dot(left, (top[...], low[...]), FLIPPED)
    out[...] = (wider(momentum[...]) + wider(gradient[...]) - product).astype(jnp.bfloat16)


def side_of(h, core):
    return h + core[0] - 2 * h * core[0]


def remembered(core, momentum, gradient, orthonormal, own, other):
    rows, half = orthonormal.shape[0], own.shape[0]
    block = pl.BlockSpec((SPAN, half), lambda h, t, core: (t, side_of(h, core)))
    whole = pl.BlockSpec((half, RANK), lambda h, t, core: (0, 0))
    split = pl.BlockSpec((half, RANK), lambda h, t, core: (h, 0))
    return pl.pallas_call(
        momentum_kernel,
        grid_spec=pltpu.PrefetchScalarGridSpec(
            num_scalar_prefetch=1,
            grid=(2, rows // SPAN),
            in_specs=[
                block,
                block,
                pl.BlockSpec((SPAN, RANK), lambda h, t, core: (t, 0)),
                whole,
                whole,
            ],
            out_specs=[block, split, split],
        ),
        out_shape=[
            jax.ShapeDtypeStruct((rows, 2 * half), jnp.bfloat16),
            jax.ShapeDtypeStruct((2 * half, RANK), jnp.bfloat16),
            jax.ShapeDtypeStruct((2 * half, RANK), jnp.bfloat16),
        ],
        cost_estimate=cost(1 << 32),
        compiler_params=pltpu.CompilerParams(vmem_limit_bytes=20 << 20),
        name="new_momentum",
    )(core, momentum, gradient, orthonormal, own, other)


def update_kernel(core, orthonormal, own, other, top, low, squares, update, basis):
    norms = jnp.sqrt(jnp.sum(squares[...], axis=0)) + eps

    @pl.when(pl.program_id(1) == 0)
    def _():
        basis[...] = jnp.where(pl.program_id(0) == 0, own[...], other[...]) / norms

    left = parts(orthonormal[...] * (math.sqrt(ROWS * COLS / RANK) / norms))
    update[...] = split_dot(left, (top[...], low[...]), FLIPPED)


def updated(core, orthonormal, own, other, top, low, squares):
    rows, half = orthonormal.shape[0], own.shape[0]
    whole = pl.BlockSpec((half, RANK), lambda h, t, core: (0, 0))
    split = pl.BlockSpec((half, RANK), lambda h, t, core: (h, 0))
    return pl.pallas_call(
        update_kernel,
        grid_spec=pltpu.PrefetchScalarGridSpec(
            num_scalar_prefetch=1,
            grid=(2, rows // SPAN),
            in_specs=[
                pl.BlockSpec((SPAN, RANK), lambda h, t, core: (t, 0)),
                whole,
                whole,
                split,
                split,
                pl.BlockSpec(squares.shape, lambda h, t, core: (0, 0, 0)),
            ],
            out_specs=[
                pl.BlockSpec((SPAN, half), lambda h, t, core: (t, side_of(h, core))),
                pl.BlockSpec((half, RANK), lambda h, t, core: (side_of(h, core), 0)),
            ],
        ),
        out_shape=[
            jax.ShapeDtypeStruct((rows, 2 * half), jnp.float32),
            jax.ShapeDtypeStruct((2 * half, RANK), jnp.float32),
        ],
        cost_estimate=cost(6 * rows * 2 * half * RANK),
        compiler_params=limit(20),
        name="update",
    )(core, orthonormal, own, other, top, low, squares)


def shards(momentum, gradient, right_basis):
    core = core_number()
    sides = lax.axis_size("x")

    part, top, low = project(momentum, gradient, right_basis)
    part, core = lax.optimization_barrier((part, core))
    own = scattered(scattered(part, "y"), "z")
    projected = gathered(gathered(own, "z"), "y")

    outgoing, kept = widen(core, top, low, projected)
    tiles = merge(core, outgoing, other_core(outgoing), kept, sides)
    tiles, gram_half = spread(lax.all_to_all(tiles, "x", 0, 0, tiled=True))
    wide_half = lax.all_to_all(tiles, "x", 0, 0, tiled=True).reshape(-1, RANK)

    inverse, orthonormal = inverted(core, gram_half, other_core(gram_half), projected)
    own, own_squares = transpose_of(wide_half, inverse, lax.axis_size(COL))
    squares = own_squares + other_core(own_squares)
    squares = lax.all_to_all(squares, COL, 0, 0, tiled=True)
    other = other_core(own)
    new_momentum, top, low = remembered(core, momentum, gradient, orthonormal, own, other)
    update, new_basis = updated(core, orthonormal, own, other, top, low, squares)
    return (new_momentum, new_basis, update)


def solution(mesh):
    split = Mesh(mesh.devices.reshape(4, 2, 8, 4), (*ROW, *COL))
    placed = (P(ROW, COL), P(ROW, COL), P(COL, None))
    return jax.shard_map(
        shards,
        mesh=split,
        in_specs=placed,
        out_specs=(P(ROW, COL), P(COL, None), P(ROW, COL)),
        check_vma=False,
    )
```

```python
import functools
import math

import jax
import jax.numpy as jnp
from jax import lax
from jax.experimental import pallas as pl
from jax.experimental.pallas import tpu as pltpu
from jax.sharding import Mesh
from jax.sharding import PartitionSpec as P

ROWS = 8192
COLS = 32768
RANK = 256
COL = ("z", "y")
ROW = ("x", "c")


eps = 1e-08
momentum_decay = 0.95


def scattered(array, axis):
    tiles = array.reshape(lax.axis_size(axis), -1, array.shape[-1])
    return lax.all_to_all(tiles, axis, 0, 0, tiled=True).sum(axis=0)


def from_everyone(array, axis):
    tiles = jnp.broadcast_to(array[None], (lax.axis_size(axis), *array.shape))
    return lax.all_to_all(tiles, axis, 0, 0, tiled=True)


def gathered(array, axis):
    return from_everyone(array, axis).reshape(-1, array.shape[-1])


def other_core(array):
    return lax.ppermute(array, "c", [(0, 1), (1, 0)])


def mxu(left, right, dims):
    return lax.dot_general(left, right, (dims, ((), ())), preferred_element_type=jnp.float32)

def parts(array):
    top = array.astype(jnp.bfloat16)
    return top, (array - top.astype(jnp.float32)).astype(jnp.bfloat16)

def dot3(left, right, dims):
    (a, b), (c, d) = parts(left), parts(right)
    return mxu(a, c, dims) + (mxu(a, d, dims) + mxu(b, c, dims))

def dot1(left, right, dims):
    return mxu(left.astype(jnp.bfloat16), right.astype(jnp.bfloat16), dims)

PLAIN = ((1,), (0,))
FLIPPED = ((1,), (1,))

def core_number():
    return lax.axis_index("c").astype(jnp.int32)[None]


def cost(flops):
    return pl.CostEstimate(flops=flops, bytes_accessed=0, transcendentals=0)


IN_VMEM = pl.BlockSpec(memory_space=pltpu.VMEM)
IN_SMEM = pl.BlockSpec(memory_space=pltpu.SMEM)
TILE = 256
HALF = RANK // 2
PACKED = 3 * HALF // 4


def wider(tile):
    return tile.astype(jnp.float32)


def split_dot(left, right, dims):
    (a, b), (c, d) = left, right
    return mxu(a, c, dims) + (mxu(a, d, dims) + mxu(b, c, dims))


def in_hbm(*arrays):
    return [pltpu.with_memory_space_constraint(a, pltpu.HBM) for a in arrays]


def limit(mib):
    return pltpu.CompilerParams(vmem_limit_bytes=mib << 20)


def both(left, right, dims):
    (a, b), (c, d) = left, right
    return (mxu(a, c, dims) + mxu(b, c, dims)) + (mxu(a, d, dims) + mxu(b, d, dims))


def project_kernel(momentum, gradient, basis, out, m, g, r, top, low, arrived):
    chunks = momentum.shape[0] // TILE
    first = pltpu.make_async_copy(basis, r, arrived.at[0])
    first.start()
    copies = []
    for t in range(chunks):
        span = pl.ds(t * TILE, TILE)
        pair = (
            pltpu.make_async_copy(momentum.at[span, :], m.at[span, :], arrived.at[2 * t + 1]),
            pltpu.make_async_copy(gradient.at[span, :], g.at[span, :], arrived.at[2 * t + 2]),
        )
        for copy in pair:
            copy.start()
        copies.append(pair)
    first.wait()
    top[...], low[...] = parts(r[...])
    for t in range(chunks):
        for copy in copies[t]:
            copy.wait()
        span = slice(t * TILE, (t + 1) * TILE)
        out[span, :] = both((m[span, :], g[span, :]), (top[...], low[...]), PLAIN)


def project(momentum, gradient, basis):
    rows, columns = momentum.shape
    return pl.pallas_call(
        project_kernel,
        in_specs=[pl.BlockSpec(memory_space=pltpu.HBM)] * 3,
        out_specs=IN_VMEM,
        out_shape=jax.ShapeDtypeStruct((rows, RANK), jnp.float32),
        scratch_shapes=[
            pltpu.VMEM((rows, columns), jnp.bfloat16),
            pltpu.VMEM((rows, columns), jnp.bfloat16),
            pltpu.VMEM((columns, RANK), jnp.float32),
            pltpu.VMEM((columns, RANK), jnp.bfloat16),
            pltpu.VMEM((columns, RANK), jnp.bfloat16),
            pltpu.SemaphoreType.DMA((2 * rows // TILE + 1,)),
        ],
        cost_estimate=cost(8 * rows * columns * RANK),
        compiler_params=limit(16),
        name="project",
    )(*in_hbm(momentum, gradient, basis))


def widen_kernel(with_gram, core, momentum, gradient, projected, out, top, low):
    half = momentum.shape[1] // 2
    top[...], low[...] = parts(projected[...].T)
    place = 1 - core[0] if with_gram else core[0]

    @pl.loop(0, half // TILE)
    def _(t):
        span = pl.ds(pl.multiple_of(place * half + t * TILE, TILE), TILE)
        pair = (momentum[:, span], gradient[:, span])
        tile = both((top[...], low[...]), pair, PLAIN)
        out[pl.ds(pl.multiple_of(t * TILE, TILE), TILE), :] = tile.T

    if with_gram:
        out[half:, :] = split_dot((top[...], low[...]), parts(projected[...]), PLAIN)


def widen(with_gram, core, momentum, gradient, projected):
    rows, columns = momentum.shape
    return pl.pallas_call(
        functools.partial(widen_kernel, with_gram),
        in_specs=[IN_SMEM, IN_VMEM, IN_VMEM, IN_VMEM],
        out_specs=IN_VMEM,
        out_shape=jax.ShapeDtypeStruct(
            (columns // 2 + (RANK if with_gram else 0), RANK), jnp.float32
        ),
        scratch_shapes=[pltpu.VMEM((RANK, rows), jnp.bfloat16)] * 2,
        cost_estimate=cost(4 * rows * columns * RANK),
        compiler_params=limit(16),
        name="widen_given" if with_gram else "widen_kept",
    )(core, momentum, gradient, projected)


def split_dot(left, right, dims):
    (a, b), (c, d) = left, right
    return mxu(a, c, dims) + (mxu(a, d, dims) + mxu(b, c, dims))


def limit(mib):
    return pltpu.CompilerParams(vmem_limit_bytes=mib << 20)


def folded(block):
    half = block.shape[0] // 2
    return jnp.concatenate((block[:half], block[half:]), axis=1)


def unfolded(block):
    return jnp.concatenate((block[:, :HALF], block[:, HALF:]), axis=0)


def merge_kernel(core, outgoing, received, kept, out):
    sides = out.shape[0]
    each = kept.shape[0] // sides
    for side in range(sides):
        span = pl.ds(side * each, each)
        out[side, :each, :] = kept[span, :] + received[span, :]
    gram = outgoing[kept.shape[0] :, :] + received[kept.shape[0] :, :]
    corner = gram[HALF:, :HALF]

    def put(square, strip):
        for side in range(sides):
            out[side, each : each + HALF // 2, :] = folded(square)
            out[side, each + HALF // 2 :, :] = folded(strip)

    @pl.when(core[0] == 0)
    def _():
        put(gram[:HALF, :HALF], corner[: HALF // 2])

    @pl.when(core[0] == 1)
    def _():
        put(gram[HALF:, HALF:], corner[HALF // 2 :])


def merge(core, outgoing, received, kept, sides):
    each = kept.shape[0] // sides
    return pl.pallas_call(
        merge_kernel,
        in_specs=[IN_SMEM, IN_VMEM, IN_VMEM, IN_VMEM],
        out_specs=IN_VMEM,
        out_shape=jax.ShapeDtypeStruct((sides, each + PACKED, RANK), jnp.float32),
        cost_estimate=cost(kept.size),
        compiler_params=pltpu.CompilerParams(vmem_limit_bytes=8 << 20),
        name="merge",
    )(core, outgoing, received, kept)


def spread_kernel(arrived, tiles, gram_half):
    sides, each, _ = tiles.shape
    wide = arrived[0, :each, :]
    gram = arrived[0, each:, :]
    for side in range(1, sides):
        wide = wide + arrived[side, :each, :]
        gram = gram + arrived[side, each:, :]
    for side in range(sides):
        tiles[side] = wide
    gram_half[...] = gram


def spread(arrived):
    sides, lines, _ = arrived.shape
    return pl.pallas_call(
        spread_kernel,
        in_specs=[IN_VMEM],
        out_specs=[IN_VMEM, IN_VMEM],
        out_shape=[
            pltpu.HBM((sides, lines - PACKED, RANK), jnp.float32),
            jax.ShapeDtypeStruct((PACKED, RANK), jnp.float32),
        ],
        cost_estimate=cost(arrived.size),
        compiler_params=limit(6),
        name="spread",
    )(arrived)


def inverse_factor(core, own, other, projected, out_ref, orthonormal, work):
    first = jnp.where(core[0] == 0, own[...], other[...])
    second = jnp.where(core[0] == 0, other[...], own[...])
    corner = jnp.concatenate((unfolded(first[HALF // 2 :]), unfolded(second[HALF // 2 :])), axis=0)
    gram = jnp.concatenate(
        (
            jnp.concatenate((unfolded(first[: HALF // 2]), corner.T), axis=1),
            jnp.concatenate((corner, unfolded(second[: HALF // 2])), axis=1),
        ),
        axis=0,
    )
    shape = (RANK, RANK)
    row, column = (lax.broadcasted_iota(jnp.int32, shape, d) for d in (0, 1))
    eye = (row == column).astype(jnp.float32)
    lower = jnp.where(row > column, 1.0, 0.5 * eye)
    diagonal = gram * eye
    along = lax.rsqrt(jnp.sum(diagonal, axis=0, keepdims=True))
    down = lax.rsqrt(jnp.sum(diagonal, axis=1, keepdims=True))
    scaled = gram * down * along

    def step(guess, dot):
        error = dot(dot(guess, scaled, PLAIN), guess, FLIPPED) - eye
        return guess - dot1(error * lower, guess, PLAIN), error

    guess = eye - (scaled - eye) * lower
    guess, _ = step(guess, dot1)
    guess, _ = step(guess, dot3)
    guess, error = step(guess, dot3)
    out_ref[...] = guess * along

    @pl.when(jnp.logical_not(jnp.sum(error * error) < 1e-4))
    def _():
        work[:, :RANK] = gram
        work[:, RANK:] = eye
        rows = lax.broadcasted_iota(jnp.int32, (RANK, 1), 0)
        lanes = lax.broadcasted_iota(jnp.int32, (1, RANK), 1)

        def eliminate(i, carry):
            line = work[pl.ds(i, 1), :]
            pivot = jnp.sum(jnp.where(lanes == i, line[:, :RANK], 0.0), axis=1, keepdims=True)
            root = lax.rsqrt(pivot)
            line = line * root
            whole = work[...]
            beneath = jnp.sum(jnp.where(lanes == i, whole[:, :RANK], 0.0), axis=1, keepdims=True) * root
            rest = whole - jnp.where(rows > i, beneath, 0.0) * line
            work[...] = jnp.where(rows == i, line, rest)
            return carry

        lax.fori_loop(0, RANK, eliminate, 0)
        out_ref[...] = jnp.where(row >= column, work[:, RANK:], 0.0)

    right = parts(out_ref[...])

    @pl.loop(0, projected.shape[0] // TILE)
    def _(t):
        span = pl.ds(pl.multiple_of(t * TILE, TILE), TILE)
        orthonormal[span, :] = split_dot(parts(projected[span, :]), right, FLIPPED)


def inverted(core, own, other, projected):
    return pl.pallas_call(
        inverse_factor,
        in_specs=[IN_SMEM, IN_VMEM, IN_VMEM, IN_VMEM],
        out_specs=[IN_VMEM, IN_VMEM],
        out_shape=[
            jax.ShapeDtypeStruct((RANK, RANK), jnp.float32),
            jax.ShapeDtypeStruct(projected.shape, jnp.float32),
        ],
        scratch_shapes=[pltpu.VMEM((RANK, 2 * RANK), jnp.float32)],
        cost_estimate=cost(1 << 32),
        compiler_params=limit(12),
        name="inverse_factor",
    )(core, own, other, projected)


def transposed_kernel(wide, inverse, out, squares):
    c, d = parts(inverse[...])
    total = jnp.zeros((1, RANK), jnp.float32)
    for t in range(wide.shape[0] // TILE):
        span = slice(t * TILE, (t + 1) * TILE)
        a, b = parts(wide[span, :])
        tile = mxu(a, c, FLIPPED) + (mxu(a, d, FLIPPED) + mxu(b, c, FLIPPED))
        out[span, :] = tile
        total += jnp.sum(tile * tile, axis=0, keepdims=True)
    squares[...] = jnp.broadcast_to(total[None], squares.shape)


def transpose_of(wide, inverse, copies):
    return pl.pallas_call(
        transposed_kernel,
        in_specs=[IN_VMEM, IN_VMEM],
        out_specs=[IN_VMEM, IN_VMEM],
        out_shape=[
            jax.ShapeDtypeStruct(wide.shape, jnp.float32),
            jax.ShapeDtypeStruct((copies, 1, RANK), jnp.float32),
        ],
        cost_estimate=cost(6 * wide.size * RANK),
        compiler_params=pltpu.CompilerParams(vmem_limit_bytes=8 << 20),
        name="transposed",
    )(wide, inverse)


SPAN = 512


def momentum_kernel(core, momentum, gradient, orthonormal, own, other, out, top, low):
    @pl.when(pl.program_id(1) == 0)
    def _():
        top[...], low[...] = parts(jnp.where(pl.program_id(0) == 0, own[...], other[...]))

    left = parts((1.0 - momentum_decay) * orthonormal[...])
    product = split_dot(left, (top[...], low[...]), FLIPPED)
    out[...] = (wider(momentum[...]) + wider(gradient[...]) - product).astype(jnp.bfloat16)


def side_of(h, core):
    return h + core[0] - 2 * h * core[0]


def remembered(core, momentum, gradient, orthonormal, own, other):
    rows, half = orthonormal.shape[0], own.shape[0]
    block = pl.BlockSpec((SPAN, half), lambda h, t, core: (t, side_of(h, core)))
    whole = pl.BlockSpec((half, RANK), lambda h, t, core: (0, 0))
    return pl.pallas_call(
        momentum_kernel,
        grid_spec=pltpu.PrefetchScalarGridSpec(
            num_scalar_prefetch=1,
            grid=(2, rows // SPAN),
            in_specs=[
                block,
                block,
                pl.BlockSpec((SPAN, RANK), lambda h, t, core: (t, 0)),
                whole,
                whole,
            ],
            out_specs=block,
            scratch_shapes=[pltpu.VMEM((half, RANK), jnp.bfloat16)] * 2,
        ),
        out_shape=jax.ShapeDtypeStruct((rows, 2 * half), jnp.bfloat16),
        cost_estimate=cost(1 << 32),
        compiler_params=pltpu.CompilerParams(vmem_limit_bytes=20 << 20),
        name="new_momentum",
    )(core, *in_hbm(momentum, gradient), orthonormal, own, other)


def update_kernel(core, orthonormal, own, other, squares, update, basis, top, low):
    norms = jnp.sqrt(jnp.sum(squares[...], axis=0)) + eps

    @pl.when(pl.program_id(1) == 0)
    def _():
        side = jnp.where(pl.program_id(0) == 0, own[...], other[...])
        top[...], low[...] = parts(side)
        basis[...] = side / norms

    left = parts(orthonormal[...] * (math.sqrt(ROWS * COLS / RANK) / norms))
    update[...] = split_dot(left, (top[...], low[...]), FLIPPED)


def updated(core, orthonormal, own, other, squares):
    rows, half = orthonormal.shape[0], own.shape[0]
    whole = pl.BlockSpec((half, RANK), lambda h, t, core: (0, 0))
    return pl.pallas_call(
        update_kernel,
        grid_spec=pltpu.PrefetchScalarGridSpec(
            num_scalar_prefetch=1,
            grid=(2, rows // SPAN),
            in_specs=[
                pl.BlockSpec((SPAN, RANK), lambda h, t, core: (t, 0)),
                whole,
                whole,
                pl.BlockSpec(squares.shape, lambda h, t, core: (0, 0, 0)),
            ],
            out_specs=[
                pl.BlockSpec((SPAN, half), lambda h, t, core: (t, side_of(h, core))),
                pl.BlockSpec((half, RANK), lambda h, t, core: (side_of(h, core), 0)),
            ],
            scratch_shapes=[pltpu.VMEM((half, RANK), jnp.bfloat16)] * 2,
        ),
        out_shape=[
            jax.ShapeDtypeStruct((rows, 2 * half), jnp.float32),
            jax.ShapeDtypeStruct((2 * half, RANK), jnp.float32),
        ],
        cost_estimate=cost(6 * rows * 2 * half * RANK),
        compiler_params=limit(20),
        name="update",
    )(core, orthonormal, own, other, squares)


def shards(momentum, gradient, right_basis):
    core = core_number()
    sides = lax.axis_size("x")

    part = project(momentum, gradient, right_basis)
    part, core = lax.optimization_barrier((part, core))
    own = scattered(scattered(part, "y"), "z")
    projected = gathered(gathered(own, "z"), "y")

    outgoing = widen(True, core, momentum, gradient, projected)
    received = other_core(outgoing)
    kept = widen(False, core, momentum, gradient, projected)
    tiles = merge(core, outgoing, received, kept, sides)
    tiles, gram_half = spread(lax.all_to_all(tiles, "x", 0, 0, tiled=True))
    wide_half = lax.all_to_all(tiles, "x", 0, 0, tiled=True).reshape(-1, RANK)

    inverse, orthonormal = inverted(core, gram_half, other_core(gram_half), projected)
    own, own_squares = transpose_of(wide_half, inverse, lax.axis_size(COL))
    squares = own_squares + other_core(own_squares)
    squares = lax.all_to_all(squares, COL, 0, 0, tiled=True)
    other = other_core(own)
    new_momentum = remembered(core, momentum, gradient, orthonormal, own, other)
    update, new_basis = updated(core, orthonormal, own, other, squares)
    return (new_momentum, new_basis, update)


def solution(mesh):
    split = Mesh(mesh.devices.reshape(4, 2, 8, 4), (*ROW, *COL))
    placed = (P(ROW, COL), P(ROW, COL), P(COL, None))
    return jax.shard_map(
        shards,
        mesh=split,
        in_specs=placed,
        out_specs=(P(ROW, COL), P(COL, None), P(ROW, COL)),
        check_vma=False,
    )
```

```python
import functools
import math

import jax
import jax.numpy as jnp
from jax import lax
from jax.experimental import pallas as pl
from jax.experimental.pallas import tpu as pltpu
from jax.sharding import Mesh
from jax.sharding import PartitionSpec as P

ROWS = 8192
COLS = 32768
RANK = 256
COL = ("z", "y")
ROW = ("x", "c")


eps = 1e-08
momentum_decay = 0.95


def scattered(array, axis):
    tiles = array.reshape(lax.axis_size(axis), -1, array.shape[-1])
    return lax.all_to_all(tiles, axis, 0, 0, tiled=True).sum(axis=0)


def from_everyone(array, axis):
    tiles = jnp.broadcast_to(array[None], (lax.axis_size(axis), *array.shape))
    return lax.all_to_all(tiles, axis, 0, 0, tiled=True)


def gathered(array, axis):
    return from_everyone(array, axis).reshape(-1, array.shape[-1])


def other_core(array):
    return lax.ppermute(array, "c", [(0, 1), (1, 0)])


def mxu(left, right, dims):
    return lax.dot_general(left, right, (dims, ((), ())), preferred_element_type=jnp.float32)

def parts(array):
    top = array.astype(jnp.bfloat16)
    return top, (array - top.astype(jnp.float32)).astype(jnp.bfloat16)

def dot3(left, right, dims):
    (a, b), (c, d) = parts(left), parts(right)
    return mxu(a, c, dims) + (mxu(a, d, dims) + mxu(b, c, dims))

def dot1(left, right, dims):
    return mxu(left.astype(jnp.bfloat16), right.astype(jnp.bfloat16), dims)

PLAIN = ((1,), (0,))
FLIPPED = ((1,), (1,))

def core_number():
    return lax.axis_index("c").astype(jnp.int32)[None]


def cost(flops):
    return pl.CostEstimate(flops=flops, bytes_accessed=0, transcendentals=0)


IN_VMEM = pl.BlockSpec(memory_space=pltpu.VMEM)
IN_SMEM = pl.BlockSpec(memory_space=pltpu.SMEM)
TILE = 256
HALF = RANK // 2
PACKED = 3 * HALF // 4


def wider(tile):
    return tile.astype(jnp.float32)


def split_dot(left, right, dims):
    (a, b), (c, d) = left, right
    return mxu(a, c, dims) + (mxu(a, d, dims) + mxu(b, c, dims))


def in_hbm(*arrays):
    return [pltpu.with_memory_space_constraint(a, pltpu.HBM) for a in arrays]


def limit(mib):
    return pltpu.CompilerParams(vmem_limit_bytes=mib << 20)


def added(product):
    return product[:, :RANK] + product[:, RANK:]


def project_kernel(momentum, gradient, basis, out, m, g, r, right, arrived):
    loads = [
        pltpu.make_async_copy(source, target, arrived.at[k])
        for k, (source, target) in enumerate(((basis, r), (momentum, m), (gradient, g)))
    ]
    for load in loads:
        load.start()
    loads[0].wait()
    right[:, :RANK], right[:, RANK:] = parts(r[...])
    spans = [slice(t, t + SPAN) for t in range(0, out.shape[0], SPAN)]
    loads[1].wait()
    for span in spans:
        out[span, :] = added(mxu(m[span, :], right[...], PLAIN))
    loads[2].wait()
    for span in spans:
        out[span, :] += added(mxu(g[span, :], right[...], PLAIN))


def project(momentum, gradient, basis):
    rows, columns = momentum.shape
    return pl.pallas_call(
        project_kernel,
        in_specs=[pl.BlockSpec(memory_space=pltpu.HBM)] * 3,
        out_specs=IN_VMEM,
        out_shape=jax.ShapeDtypeStruct((rows, RANK), jnp.float32),
        scratch_shapes=[
            pltpu.VMEM((rows, columns), jnp.bfloat16),
            pltpu.VMEM((rows, columns), jnp.bfloat16),
            pltpu.VMEM((columns, RANK), jnp.float32),
            pltpu.VMEM((columns, 2 * RANK), jnp.bfloat16),
            pltpu.SemaphoreType.DMA((3,)),
        ],
        cost_estimate=cost(8 * rows * columns * RANK),
        compiler_params=limit(16),
        name="project",
    )(*in_hbm(momentum, gradient, basis))


def widen_kernel(with_gram, core, momentum, gradient, projected, out, left):
    half = momentum.shape[1] // 2
    left[:RANK, :], left[RANK:, :] = parts(projected[...].T)
    place = 1 - core[0] if with_gram else core[0]
    span = pl.ds(pl.multiple_of(place * half, half), half)
    product = mxu(left[...], momentum[:, span], PLAIN) + mxu(left[...], gradient[:, span], PLAIN)
    out[:half, :] = (product[:RANK] + product[RANK:]).T

    if with_gram:
        top, low = parts(projected[...])
        product = mxu(left[...], top, PLAIN)
        out[half:, :] = product[:RANK] + (product[RANK:] + mxu(left[:RANK, :], low, PLAIN))


def widen(with_gram, core, momentum, gradient, projected):
    rows, columns = momentum.shape
    return pl.pallas_call(
        functools.partial(widen_kernel, with_gram),
        in_specs=[IN_SMEM, IN_VMEM, IN_VMEM, IN_VMEM],
        out_specs=IN_VMEM,
        out_shape=jax.ShapeDtypeStruct(
            (columns // 2 + (RANK if with_gram else 0), RANK), jnp.float32
        ),
        scratch_shapes=[pltpu.VMEM((2 * RANK, rows), jnp.bfloat16)],
        cost_estimate=cost(4 * rows * columns * RANK),
        compiler_params=limit(16),
        name="widen_given" if with_gram else "widen_kept",
    )(core, momentum, gradient, projected)


def split_dot(left, right, dims):
    (a, b), (c, d) = left, right
    return mxu(a, c, dims) + (mxu(a, d, dims) + mxu(b, c, dims))


def limit(mib):
    return pltpu.CompilerParams(vmem_limit_bytes=mib << 20)


def folded(block):
    half = block.shape[0] // 2
    return jnp.concatenate((block[:half], block[half:]), axis=1)


def unfolded(block):
    return jnp.concatenate((block[:, :HALF], block[:, HALF:]), axis=0)


def merge_kernel(core, outgoing, received, kept, out):
    sides = out.shape[0]
    each = kept.shape[0] // sides
    for side in range(sides):
        span = pl.ds(side * each, each)
        out[side, :each, :] = kept[span, :] + received[span, :]
    gram = outgoing[kept.shape[0] :, :] + received[kept.shape[0] :, :]
    corner = gram[HALF:, :HALF]

    def put(square, strip):
        for side in range(sides):
            out[side, each : each + HALF // 2, :] = folded(square)
            out[side, each + HALF // 2 :, :] = folded(strip)

    @pl.when(core[0] == 0)
    def _():
        put(gram[:HALF, :HALF], corner[: HALF // 2])

    @pl.when(core[0] == 1)
    def _():
        put(gram[HALF:, HALF:], corner[HALF // 2 :])


def merge(core, outgoing, received, kept, sides):
    each = kept.shape[0] // sides
    return pl.pallas_call(
        merge_kernel,
        in_specs=[IN_SMEM, IN_VMEM, IN_VMEM, IN_VMEM],
        out_specs=IN_VMEM,
        out_shape=jax.ShapeDtypeStruct((sides, each + PACKED, RANK), jnp.float32),
        cost_estimate=cost(kept.size),
        compiler_params=pltpu.CompilerParams(vmem_limit_bytes=8 << 20),
        name="merge",
    )(core, outgoing, received, kept)


def spread_kernel(arrived, tiles, gram_half):
    sides, each, _ = tiles.shape
    wide = arrived[0, :each, :]
    gram = arrived[0, each:, :]
    for side in range(1, sides):
        wide = wide + arrived[side, :each, :]
        gram = gram + arrived[side, each:, :]
    for side in range(sides):
        tiles[side] = wide
    gram_half[...] = gram


def spread(arrived):
    sides, lines, _ = arrived.shape
    return pl.pallas_call(
        spread_kernel,
        in_specs=[IN_VMEM],
        out_specs=[IN_VMEM, IN_VMEM],
        out_shape=[
            pltpu.HBM((sides, lines - PACKED, RANK), jnp.float32),
            jax.ShapeDtypeStruct((PACKED, RANK), jnp.float32),
        ],
        cost_estimate=cost(arrived.size),
        compiler_params=limit(6),
        name="spread",
    )(arrived)


def inverse_factor(core, own, other, projected, out_ref, orthonormal, work):
    first = jnp.where(core[0] == 0, own[...], other[...])
    second = jnp.where(core[0] == 0, other[...], own[...])
    corner = jnp.concatenate((unfolded(first[HALF // 2 :]), unfolded(second[HALF // 2 :])), axis=0)
    gram = jnp.concatenate(
        (
            jnp.concatenate((unfolded(first[: HALF // 2]), corner.T), axis=1),
            jnp.concatenate((corner, unfolded(second[: HALF // 2])), axis=1),
        ),
        axis=0,
    )
    shape = (RANK, RANK)
    row, column = (lax.broadcasted_iota(jnp.int32, shape, d) for d in (0, 1))
    eye = (row == column).astype(jnp.float32)
    lower = jnp.where(row > column, 1.0, 0.5 * eye)
    diagonal = gram * eye
    along = lax.rsqrt(jnp.sum(diagonal, axis=0, keepdims=True))
    down = lax.rsqrt(jnp.sum(diagonal, axis=1, keepdims=True))
    scaled = gram * down * along

    def step(guess, dot):
        error = dot(dot(guess, scaled, PLAIN), guess, FLIPPED) - eye
        return guess - dot1(error * lower, guess, PLAIN), error

    guess = eye - (scaled - eye) * lower
    guess, _ = step(guess, dot1)
    guess, _ = step(guess, dot3)
    guess, error = step(guess, dot3)
    out_ref[...] = guess * along

    @pl.when(jnp.logical_not(jnp.sum(error * error) < 1e-4))
    def _():
        work[:, :RANK] = gram
        work[:, RANK:] = eye
        rows = lax.broadcasted_iota(jnp.int32, (RANK, 1), 0)
        lanes = lax.broadcasted_iota(jnp.int32, (1, RANK), 1)

        def eliminate(i, carry):
            line = work[pl.ds(i, 1), :]
            pivot = jnp.sum(jnp.where(lanes == i, line[:, :RANK], 0.0), axis=1, keepdims=True)
            root = lax.rsqrt(pivot)
            line = line * root
            whole = work[...]
            beneath = jnp.sum(jnp.where(lanes == i, whole[:, :RANK], 0.0), axis=1, keepdims=True) * root
            rest = whole - jnp.where(rows > i, beneath, 0.0) * line
            work[...] = jnp.where(rows == i, line, rest)
            return carry

        lax.fori_loop(0, RANK, eliminate, 0)
        out_ref[...] = jnp.where(row >= column, work[:, RANK:], 0.0)

    right = parts(out_ref[...])

    @pl.loop(0, projected.shape[0] // TILE)
    def _(t):
        span = pl.ds(pl.multiple_of(t * TILE, TILE), TILE)
        orthonormal[span, :] = split_dot(parts(projected[span, :]), right, FLIPPED)


def inverted(core, own, other, projected):
    return pl.pallas_call(
        inverse_factor,
        in_specs=[IN_SMEM, IN_VMEM, IN_VMEM, IN_VMEM],
        out_specs=[IN_VMEM, IN_VMEM],
        out_shape=[
            jax.ShapeDtypeStruct((RANK, RANK), jnp.float32),
            jax.ShapeDtypeStruct(projected.shape, jnp.float32),
        ],
        scratch_shapes=[pltpu.VMEM((RANK, 2 * RANK), jnp.float32)],
        cost_estimate=cost(1 << 32),
        compiler_params=limit(12),
        name="inverse_factor",
    )(core, own, other, projected)


def transposed_kernel(wide, inverse, out, squares):
    c, d = parts(inverse[...])
    total = jnp.zeros((1, RANK), jnp.float32)
    for t in range(wide.shape[0] // TILE):
        span = slice(t * TILE, (t + 1) * TILE)
        a, b = parts(wide[span, :])
        tile = mxu(a, c, FLIPPED) + (mxu(a, d, FLIPPED) + mxu(b, c, FLIPPED))
        out[span, :] = tile
        total += jnp.sum(tile * tile, axis=0, keepdims=True)
    squares[...] = jnp.broadcast_to(total[None], squares.shape)


def transpose_of(wide, inverse, copies):
    return pl.pallas_call(
        transposed_kernel,
        in_specs=[IN_VMEM, IN_VMEM],
        out_specs=[IN_VMEM, IN_VMEM],
        out_shape=[
            jax.ShapeDtypeStruct(wide.shape, jnp.float32),
            jax.ShapeDtypeStruct((copies, 1, RANK), jnp.float32),
        ],
        cost_estimate=cost(6 * wide.size * RANK),
        compiler_params=pltpu.CompilerParams(vmem_limit_bytes=8 << 20),
        name="transposed",
    )(wide, inverse)


SPAN = 512


def momentum_kernel(core, momentum, gradient, orthonormal, own, other, out, top, low):
    @pl.when(pl.program_id(1) == 0)
    def _():
        top[...], low[...] = parts(jnp.where(pl.program_id(0) == 0, own[...], other[...]))

    left = parts((1.0 - momentum_decay) * orthonormal[...])
    product = split_dot(left, (top[...], low[...]), FLIPPED)
    out[...] = (wider(momentum[...]) + wider(gradient[...]) - product).astype(jnp.bfloat16)


def side_of(h, core):
    return h + core[0] - 2 * h * core[0]


def remembered(core, momentum, gradient, orthonormal, own, other):
    rows, half = orthonormal.shape[0], own.shape[0]
    block = pl.BlockSpec((SPAN, half), lambda h, t, core: (t, side_of(h, core)))
    whole = pl.BlockSpec((half, RANK), lambda h, t, core: (0, 0))
    return pl.pallas_call(
        momentum_kernel,
        grid_spec=pltpu.PrefetchScalarGridSpec(
            num_scalar_prefetch=1,
            grid=(2, rows // SPAN),
            in_specs=[
                block,
                block,
                pl.BlockSpec((SPAN, RANK), lambda h, t, core: (t, 0)),
                whole,
                whole,
            ],
            out_specs=block,
            scratch_shapes=[pltpu.VMEM((half, RANK), jnp.bfloat16)] * 2,
        ),
        out_shape=jax.ShapeDtypeStruct((rows, 2 * half), jnp.bfloat16),
        cost_estimate=cost(1 << 32),
        compiler_params=pltpu.CompilerParams(vmem_limit_bytes=20 << 20),
        name="new_momentum",
    )(core, *in_hbm(momentum, gradient), orthonormal, own, other)


def update_kernel(core, orthonormal, own, other, squares, update, basis, top, low):
    norms = jnp.sqrt(jnp.sum(squares[...], axis=0)) + eps

    @pl.when(pl.program_id(1) == 0)
    def _():
        side = jnp.where(pl.program_id(0) == 0, own[...], other[...])
        top[...], low[...] = parts(side)
        basis[...] = side / norms

    left = parts(orthonormal[...] * (math.sqrt(ROWS * COLS / RANK) / norms))
    update[...] = split_dot(left, (top[...], low[...]), FLIPPED)


def updated(core, orthonormal, own, other, squares):
    rows, half = orthonormal.shape[0], own.shape[0]
    whole = pl.BlockSpec((half, RANK), lambda h, t, core: (0, 0))
    return pl.pallas_call(
        update_kernel,
        grid_spec=pltpu.PrefetchScalarGridSpec(
            num_scalar_prefetch=1,
            grid=(2, 1),
            in_specs=[
                pl.BlockSpec((rows, RANK), lambda h, t, core: (t, 0)),
                whole,
                whole,
                pl.BlockSpec(squares.shape, lambda h, t, core: (0, 0, 0)),
            ],
            out_specs=[
                pl.BlockSpec((rows, half), lambda h, t, core: (t, side_of(h, core))),
                pl.BlockSpec((half, RANK), lambda h, t, core: (side_of(h, core), 0)),
            ],
            scratch_shapes=[pltpu.VMEM((half, RANK), jnp.bfloat16)] * 2,
        ),
        out_shape=[
            jax.ShapeDtypeStruct((rows, 2 * half), jnp.float32),
            jax.ShapeDtypeStruct((2 * half, RANK), jnp.float32),
        ],
        cost_estimate=cost(6 * rows * 2 * half * RANK),
        compiler_params=limit(20),
        name="update",
    )(core, orthonormal, own, other, squares)


def shards(momentum, gradient, right_basis):
    core = core_number()
    sides = lax.axis_size("x")

    part = project(momentum, gradient, right_basis)
    part, core = lax.optimization_barrier((part, core))
    own = scattered(scattered(part, "y"), "z")
    projected = gathered(gathered(own, "z"), "y")

    outgoing = widen(True, core, momentum, gradient, projected)
    received = other_core(outgoing)
    kept = widen(False, core, momentum, gradient, projected)
    tiles = merge(core, outgoing, received, kept, sides)
    tiles, gram_half = spread(lax.all_to_all(tiles, "x", 0, 0, tiled=True))
    wide_half = lax.all_to_all(tiles, "x", 0, 0, tiled=True).reshape(-1, RANK)

    inverse, orthonormal = inverted(core, gram_half, other_core(gram_half), projected)
    everyone = ("c", *COL)
    own, squares = transpose_of(wide_half, inverse, lax.axis_size(everyone))
    squares = lax.all_to_all(squares, everyone, 0, 0, tiled=True)
    other = other_core(own)
    new_momentum = remembered(core, momentum, gradient, orthonormal, own, other)
    update, new_basis = updated(core, orthonormal, own, other, squares)
    return (new_momentum, new_basis, update)


def solution(mesh):
    split = Mesh(mesh.devices.reshape(4, 2, 8, 4), (*ROW, *COL))
    placed = (P(ROW, COL), P(ROW, COL), P(COL, None))
    return jax.shard_map(
        shards,
        mesh=split,
        in_specs=placed,
        out_specs=(P(ROW, COL), P(COL, None), P(ROW, COL)),
        check_vma=False,
    )
```

```python
import functools
import math

import jax
import jax.numpy as jnp
from jax import lax
from jax.experimental import pallas as pl
from jax.experimental.pallas import tpu as pltpu
from jax.sharding import Mesh
from jax.sharding import PartitionSpec as P

ROWS = 8192
COLS = 32768
RANK = 256
COL = ("z", "y")
ROW = ("x", "c")


eps = 1e-08
momentum_decay = 0.95


def scattered(array, axis):
    tiles = array.reshape(lax.axis_size(axis), -1, array.shape[-1])
    return lax.all_to_all(tiles, axis, 0, 0, tiled=True).sum(axis=0)


def from_everyone(array, axis):
    tiles = jnp.broadcast_to(array[None], (lax.axis_size(axis), *array.shape))
    return lax.all_to_all(tiles, axis, 0, 0, tiled=True)


def gathered(array, axis):
    return from_everyone(array, axis).reshape(-1, array.shape[-1])


def other_core(array):
    return lax.ppermute(array, "c", [(0, 1), (1, 0)])


def mxu(left, right, dims):
    return lax.dot_general(left, right, (dims, ((), ())), preferred_element_type=jnp.float32)


def parts(array):
    top = array.astype(jnp.bfloat16)
    return top, (array - top.astype(jnp.float32)).astype(jnp.bfloat16)


def dot3(left, right, dims):
    (a, b), (c, d) = parts(left), parts(right)
    return mxu(a, c, dims) + (mxu(a, d, dims) + mxu(b, c, dims))


def dot1(left, right, dims):
    return mxu(left.astype(jnp.bfloat16), right.astype(jnp.bfloat16), dims)


PLAIN = ((1,), (0,))
FLIPPED = ((1,), (1,))


def place_on(axis):
    return lax.axis_index(axis).astype(jnp.int32)[None]


def from_others(array, axis):
    length = lax.axis_size(axis)
    rings = ([(i, (i + k) % length) for i in range(length)] for k in range(1, length))
    return [array, *(lax.ppermute(array, axis, ring) for ring in rings)]


def origin(place, k, length):
    return lax.rem(place + length - k, length)


def cost(flops):
    return pl.CostEstimate(flops=flops, bytes_accessed=0, transcendentals=0)


IN_VMEM = pl.BlockSpec(memory_space=pltpu.VMEM)
IN_SMEM = pl.BlockSpec(memory_space=pltpu.SMEM)
TILE = 256
HALF = RANK // 2


def wider(tile):
    return tile.astype(jnp.float32)


def split_dot(left, right, dims):
    (a, b), (c, d) = left, right
    return mxu(a, c, dims) + (mxu(a, d, dims) + mxu(b, c, dims))


def in_hbm(*arrays):
    return [pltpu.with_memory_space_constraint(a, pltpu.HBM) for a in arrays]


def limit(mib):
    return pltpu.CompilerParams(vmem_limit_bytes=mib << 20)


def added(product):
    return product[:, :RANK] + product[:, RANK:]


def project_kernel(momentum, gradient, basis, out, m, g, r, right, arrived):
    loads = [
        pltpu.make_async_copy(source, target, arrived.at[k])
        for k, (source, target) in enumerate(((basis, r), (momentum, m), (gradient, g)))
    ]
    for load in loads:
        load.start()
    loads[0].wait()
    right[:, :RANK], right[:, RANK:] = parts(r[...])
    spans = [slice(t, t + SPAN) for t in range(0, out.shape[0], SPAN)]
    loads[1].wait()
    for span in spans:
        out[span, :] = added(mxu(m[span, :], right[...], PLAIN))
    loads[2].wait()
    for span in spans:
        out[span, :] += added(mxu(g[span, :], right[...], PLAIN))


def project(momentum, gradient, basis):
    rows, columns = momentum.shape
    return pl.pallas_call(
        project_kernel,
        in_specs=[pl.BlockSpec(memory_space=pltpu.HBM)] * 3,
        out_specs=IN_VMEM,
        out_shape=jax.ShapeDtypeStruct((rows, RANK), jnp.float32),
        scratch_shapes=[
            pltpu.VMEM((rows, columns), jnp.bfloat16),
            pltpu.VMEM((rows, columns), jnp.bfloat16),
            pltpu.VMEM((columns, RANK), jnp.float32),
            pltpu.VMEM((columns, 2 * RANK), jnp.bfloat16),
            pltpu.SemaphoreType.DMA((3,)),
        ],
        cost_estimate=cost(8 * rows * columns * RANK),
        compiler_params=limit(16),
        name="project",
    )(*in_hbm(momentum, gradient, basis))


def widen_kernel(give, core, line, momentum, gradient, *refs):
    *chunks, out, left = refs
    half = momentum.shape[1] // 2
    for k, chunk in enumerate(chunks):
        top, low = parts(chunk[...].T)
        start = origin(line[0], k, len(chunks)) * chunk.shape[0]
        span = pl.ds(pl.multiple_of(start, TILE), chunk.shape[0])
        left[:RANK, span] = top
        left[RANK:, span] = low
    place = 1 - core[0] if give else core[0]
    span = pl.ds(pl.multiple_of(place * half, half), half)
    product = mxu(left[...], momentum[:, span], PLAIN) + mxu(left[...], gradient[:, span], PLAIN)
    out[...] = (product[:RANK] + product[RANK:]).T


def widen(give, core, line, momentum, gradient, chunks):
    rows, columns = momentum.shape
    return pl.pallas_call(
        functools.partial(widen_kernel, give),
        in_specs=[IN_SMEM, IN_SMEM] + [IN_VMEM] * (2 + len(chunks)),
        out_specs=IN_VMEM,
        out_shape=jax.ShapeDtypeStruct((columns // 2, RANK), jnp.float32),
        scratch_shapes=[pltpu.VMEM((2 * RANK, rows), jnp.bfloat16)],
        cost_estimate=cost(4 * rows * columns * RANK),
        compiler_params=limit(16),
        name="widen_given" if give else "widen_kept",
    )(core, line, momentum, gradient, *chunks)


def gram_kernel(chunk, out):
    flat = parts(chunk[...].T)
    out[...] = split_dot(flat, parts(chunk[...]), PLAIN)


def gram_of(chunk):
    return pl.pallas_call(
        gram_kernel,
        in_specs=[IN_VMEM],
        out_specs=IN_VMEM,
        out_shape=jax.ShapeDtypeStruct((RANK, RANK), jnp.float32),
        cost_estimate=cost(6 * chunk.size * RANK),
        compiler_params=limit(6),
        name="gram",
    )(chunk)


def split_dot(left, right, dims):
    (a, b), (c, d) = left, right
    return mxu(a, c, dims) + (mxu(a, d, dims) + mxu(b, c, dims))


def limit(mib):
    return pltpu.CompilerParams(vmem_limit_bytes=mib << 20)


def inverse_factor(line, gram_ref, *refs):
    *chunks, out_ref, orthonormal, work = refs
    gram = gram_ref[...]
    shape = (RANK, RANK)
    row, column = (lax.broadcasted_iota(jnp.int32, shape, d) for d in (0, 1))
    eye = (row == column).astype(jnp.float32)
    lower = jnp.where(row > column, 1.0, 0.5 * eye)
    diagonal = gram * eye
    along = lax.rsqrt(jnp.sum(diagonal, axis=0, keepdims=True))
    down = lax.rsqrt(jnp.sum(diagonal, axis=1, keepdims=True))
    scaled = gram * down * along

    def step(guess, dot):
        error = dot(dot(guess, scaled, PLAIN), guess, FLIPPED) - eye
        return guess - dot1(error * lower, guess, PLAIN), error

    guess = eye - (scaled - eye) * lower
    guess, _ = step(guess, dot1)
    guess, _ = step(guess, dot3)
    guess, error = step(guess, dot3)
    out_ref[...] = guess * along

    @pl.when(jnp.logical_not(jnp.sum(error * error) < 1e-4))
    def _():
        work[:, :RANK] = gram
        work[:, RANK:] = eye
        rows = lax.broadcasted_iota(jnp.int32, (RANK, 1), 0)
        lanes = lax.broadcasted_iota(jnp.int32, (1, RANK), 1)

        def eliminate(i, carry):
            line = work[pl.ds(i, 1), :]
            pivot = jnp.sum(jnp.where(lanes == i, line[:, :RANK], 0.0), axis=1, keepdims=True)
            root = lax.rsqrt(pivot)
            line = line * root
            whole = work[...]
            beneath = jnp.sum(jnp.where(lanes == i, whole[:, :RANK], 0.0), axis=1, keepdims=True) * root
            rest = whole - jnp.where(rows > i, beneath, 0.0) * line
            work[...] = jnp.where(rows == i, line, rest)
            return carry

        lax.fori_loop(0, RANK, eliminate, 0)
        out_ref[...] = jnp.where(row >= column, work[:, RANK:], 0.0)

    right = parts(out_ref[...])
    for k, chunk in enumerate(chunks):
        start = origin(line[0], k, len(chunks)) * chunk.shape[0]
        span = pl.ds(pl.multiple_of(start, TILE), chunk.shape[0])
        orthonormal[span, :] = split_dot(parts(chunk[...]), right, FLIPPED)


def inverted(line, gram, chunks):
    rows = len(chunks) * chunks[0].shape[0]
    return pl.pallas_call(
        inverse_factor,
        in_specs=[IN_SMEM] + [IN_VMEM] * (1 + len(chunks)),
        out_specs=[IN_VMEM, IN_VMEM],
        out_shape=[
            jax.ShapeDtypeStruct((RANK, RANK), jnp.float32),
            jax.ShapeDtypeStruct((rows, RANK), jnp.float32),
        ],
        scratch_shapes=[pltpu.VMEM((RANK, 2 * RANK), jnp.float32)],
        cost_estimate=cost(1 << 32),
        compiler_params=limit(12),
        name="inverse_factor",
    )(line, gram, *chunks)


def transposed_kernel(arrived, inverse, out, squares):
    wide = arrived[0]
    for side in range(1, arrived.shape[0]):
        wide = wide + arrived[side]
    tile = split_dot(parts(wide), parts(inverse[...]), FLIPPED)
    out[...] = tile
    total = jnp.sum(tile * tile, axis=0, keepdims=True)
    squares[...] = jnp.broadcast_to(total[None], squares.shape)


def transpose_of(arrived, inverse, copies):
    return pl.pallas_call(
        transposed_kernel,
        in_specs=[IN_VMEM, IN_VMEM],
        out_specs=[IN_VMEM, IN_VMEM],
        out_shape=[
            jax.ShapeDtypeStruct(arrived.shape[1:], jnp.float32),
            pltpu.HBM((copies, 1, RANK), jnp.float32),
        ],
        cost_estimate=cost(6 * arrived.size * RANK),
        compiler_params=limit(8),
        name="transposed",
    )(arrived, inverse)


def assemble_kernel(line, *refs):
    *pieces, out = refs
    for k, piece in enumerate(pieces):
        start = origin(line[0], k, len(pieces)) * piece.shape[0]
        out[pl.ds(pl.multiple_of(start, HALF), piece.shape[0]), :] = piece[...]


def assembled(line, pieces):
    rows = len(pieces) * pieces[0].shape[0]
    return pl.pallas_call(
        assemble_kernel,
        in_specs=[IN_SMEM] + [IN_VMEM] * len(pieces),
        out_specs=IN_VMEM,
        out_shape=jax.ShapeDtypeStruct((rows, RANK), jnp.float32),
        cost_estimate=cost(rows * RANK),
        compiler_params=limit(6),
        name="assembled",
    )(line, *pieces)


SPAN = 512


def momentum_kernel(core, momentum, gradient, orthonormal, own, other, out, top, low):
    @pl.when(pl.program_id(1) == 0)
    def _():
        top[...], low[...] = parts(jnp.where(pl.program_id(0) == 0, own[...], other[...]))

    left = parts((1.0 - momentum_decay) * orthonormal[...])
    product = split_dot(left, (top[...], low[...]), FLIPPED)
    out[...] = (wider(momentum[...]) + wider(gradient[...]) - product).astype(jnp.bfloat16)


def side_of(h, core):
    return h + core[0] - 2 * h * core[0]


def remembered(core, momentum, gradient, orthonormal, own, other):
    rows, half = orthonormal.shape[0], own.shape[0]
    block = pl.BlockSpec((SPAN, half), lambda h, t, core: (t, side_of(h, core)))
    whole = pl.BlockSpec((half, RANK), lambda h, t, core: (0, 0))
    return pl.pallas_call(
        momentum_kernel,
        grid_spec=pltpu.PrefetchScalarGridSpec(
            num_scalar_prefetch=1,
            grid=(2, rows // SPAN),
            in_specs=[
                block,
                block,
                pl.BlockSpec((SPAN, RANK), lambda h, t, core: (t, 0)),
                whole,
                whole,
            ],
            out_specs=block,
            scratch_shapes=[pltpu.VMEM((half, RANK), jnp.bfloat16)] * 2,
        ),
        out_shape=jax.ShapeDtypeStruct((rows, 2 * half), jnp.bfloat16),
        cost_estimate=cost(1 << 32),
        compiler_params=pltpu.CompilerParams(vmem_limit_bytes=20 << 20),
        name="new_momentum",
    )(core, *in_hbm(momentum, gradient), orthonormal, own, other)


def update_kernel(core, orthonormal, own, other, squares, update, basis, top, low):
    norms = jnp.sqrt(jnp.sum(squares[...], axis=0)) + eps

    @pl.when(pl.program_id(1) == 0)
    def _():
        side = jnp.where(pl.program_id(0) == 0, own[...], other[...])
        top[...], low[...] = parts(side)
        basis[...] = side / norms

    left = parts(orthonormal[...] * (math.sqrt(ROWS * COLS / RANK) / norms))
    update[...] = split_dot(left, (top[...], low[...]), FLIPPED)


def updated(core, orthonormal, own, other, squares):
    rows, half = orthonormal.shape[0], own.shape[0]
    whole = pl.BlockSpec((half, RANK), lambda h, t, core: (0, 0))
    return pl.pallas_call(
        update_kernel,
        grid_spec=pltpu.PrefetchScalarGridSpec(
            num_scalar_prefetch=1,
            grid=(2, 1),
            in_specs=[
                pl.BlockSpec((rows, RANK), lambda h, t, core: (t, 0)),
                whole,
                whole,
                pl.BlockSpec(squares.shape, lambda h, t, core: (0, 0, 0)),
            ],
            out_specs=[
                pl.BlockSpec((rows, half), lambda h, t, core: (t, side_of(h, core))),
                pl.BlockSpec((half, RANK), lambda h, t, core: (side_of(h, core), 0)),
            ],
            scratch_shapes=[pltpu.VMEM((half, RANK), jnp.bfloat16)] * 2,
        ),
        out_shape=[
            jax.ShapeDtypeStruct((rows, 2 * half), jnp.float32),
            jax.ShapeDtypeStruct((2 * half, RANK), jnp.float32),
        ],
        cost_estimate=cost(6 * rows * 2 * half * RANK),
        compiler_params=limit(20),
        name="update",
    )(core, orthonormal, own, other, squares)


def step(momentum, gradient, right_basis):
    core, line, side = place_on("c"), place_on("y"), place_on("x")
    sides = lax.axis_size("x")

    part = project(momentum, gradient, right_basis)
    own = scattered(scattered(part, "y"), "z")
    chunk = gathered(own, "z")
    chunks = from_others(chunk, "y")

    piece = scattered(gram_of(chunk), ("x", "y"))
    gram_matrix = gathered(piece + other_core(piece), ("x", "y"))
    inverse, orthonormal = inverted(line, gram_matrix, chunks)

    received = other_core(widen(True, core, line, momentum, gradient, chunks))
    wide = widen(False, core, line, momentum, gradient, chunks) + received
    arrived = lax.all_to_all(wide.reshape(sides, -1, RANK), "x", 0, 0, tiled=True)

    piece, squares = transpose_of(arrived, inverse, lax.axis_size((*ROW, *COL)))
    pieces = from_others(piece, "x")
    squares = lax.all_to_all(squares, (*ROW, *COL), 0, 0, tiled=True)
    own = assembled(side, pieces)
    other = other_core(own)
    new_momentum = remembered(core, momentum, gradient, orthonormal, own, other)
    update, new_basis = updated(core, orthonormal, own, other, squares)
    return (new_momentum, new_basis, update)


def solution(mesh):
    split = Mesh(mesh.devices.reshape(4, 2, 8, 4), (*ROW, *COL))
    placed = (P(ROW, COL), P(ROW, COL), P(COL, None))
    return jax.shard_map(
        step,
        mesh=split,
        in_specs=placed,
        out_specs=(P(ROW, COL), P(COL, None), P(ROW, COL)),
        check_vma=False,
    )
```

```python
import functools
import math

import jax
import jax.numpy as jnp
from jax import lax
from jax.experimental import pallas as pl
from jax.experimental.pallas import tpu as pltpu
from jax.sharding import Mesh
from jax.sharding import PartitionSpec as P

ROWS = 8192
COLS = 32768
RANK = 256
COL = ("z", "y")
ROW = ("x", "c")


eps = 1e-08
momentum_decay = 0.95


def scattered(array, axis):
    tiles = array.reshape(lax.axis_size(axis), -1, array.shape[-1])
    return lax.all_to_all(tiles, axis, 0, 0, tiled=True).sum(axis=0)


def from_everyone(array, axis):
    tiles = jnp.broadcast_to(array[None], (lax.axis_size(axis), *array.shape))
    return lax.all_to_all(tiles, axis, 0, 0, tiled=True)


def gathered(array, axis):
    return from_everyone(array, axis).reshape(-1, array.shape[-1])


def other_core(array):
    return lax.ppermute(array, "c", [(0, 1), (1, 0)])


def mxu(left, right, dims):
    return lax.dot_general(left, right, (dims, ((), ())), preferred_element_type=jnp.float32)


def parts(array):
    top = array.astype(jnp.bfloat16)
    return top, (array - top.astype(jnp.float32)).astype(jnp.bfloat16)


def dot3(left, right, dims):
    (a, b), (c, d) = parts(left), parts(right)
    return mxu(a, c, dims) + (mxu(a, d, dims) + mxu(b, c, dims))


def dot1(left, right, dims):
    return mxu(left.astype(jnp.bfloat16), right.astype(jnp.bfloat16), dims)


PLAIN = ((1,), (0,))
FLIPPED = ((1,), (1,))


def place_on(axis):
    return lax.axis_index(axis).astype(jnp.int32)[None]


def from_others(array, axis):
    length = lax.axis_size(axis)
    rings = ([(i, (i + k) % length) for i in range(length)] for k in range(1, length))
    return [array, *(lax.ppermute(array, axis, ring) for ring in rings)]


def cost(flops):
    return pl.CostEstimate(flops=flops, bytes_accessed=0, transcendentals=0)


IN_VMEM = pl.BlockSpec(memory_space=pltpu.VMEM)
IN_SMEM = pl.BlockSpec(memory_space=pltpu.SMEM)
TILE = 256
HALF = RANK // 2
PACKED = 3 * HALF // 4


def wider(tile):
    return tile.astype(jnp.float32)


def split_dot(left, right, dims):
    (a, b), (c, d) = left, right
    return mxu(a, c, dims) + (mxu(a, d, dims) + mxu(b, c, dims))


def in_hbm(*arrays):
    return [pltpu.with_memory_space_constraint(a, pltpu.HBM) for a in arrays]


def limit(mib):
    return pltpu.CompilerParams(vmem_limit_bytes=mib << 20)


def added(product):
    return product[:, :RANK] + product[:, RANK:]


def project_kernel(momentum, gradient, basis, out, m, g, r, right, arrived):
    loads = [
        pltpu.make_async_copy(source, target, arrived.at[k])
        for k, (source, target) in enumerate(((basis, r), (momentum, m), (gradient, g)))
    ]
    for load in loads:
        load.start()
    loads[0].wait()
    right[:, :RANK], right[:, RANK:] = parts(r[...])
    spans = [slice(t, t + SPAN) for t in range(0, out.shape[0], SPAN)]
    loads[1].wait()
    for span in spans:
        out[span, :] = added(mxu(m[span, :], right[...], PLAIN))
    loads[2].wait()
    for span in spans:
        out[span, :] += added(mxu(g[span, :], right[...], PLAIN))


def project(momentum, gradient, basis):
    rows, columns = momentum.shape
    return pl.pallas_call(
        project_kernel,
        in_specs=[pl.BlockSpec(memory_space=pltpu.HBM)] * 3,
        out_specs=IN_VMEM,
        out_shape=jax.ShapeDtypeStruct((rows, RANK), jnp.float32),
        scratch_shapes=[
            pltpu.VMEM((rows, columns), jnp.bfloat16),
            pltpu.VMEM((rows, columns), jnp.bfloat16),
            pltpu.VMEM((columns, RANK), jnp.float32),
            pltpu.VMEM((columns, 2 * RANK), jnp.bfloat16),
            pltpu.SemaphoreType.DMA((3,)),
        ],
        cost_estimate=cost(8 * rows * columns * RANK),
        compiler_params=limit(16),
        name="project",
    )(*in_hbm(momentum, gradient, basis))


def widen_kernel(with_gram, core, momentum, gradient, projected, out, left):
    half = momentum.shape[1] // 2
    left[:RANK, :], left[RANK:, :] = parts(projected[...].T)
    place = 1 - core[0] if with_gram else core[0]
    span = pl.ds(pl.multiple_of(place * half, half), half)
    product = mxu(left[...], momentum[:, span], PLAIN) + mxu(left[...], gradient[:, span], PLAIN)
    out[:half, :] = (product[:RANK] + product[RANK:]).T

    if with_gram:
        top, low = parts(projected[...])
        product = mxu(left[...], top, PLAIN)
        out[half:, :] = product[:RANK] + (product[RANK:] + mxu(left[:RANK, :], low, PLAIN))


def widen(with_gram, core, momentum, gradient, projected):
    rows, columns = momentum.shape
    return pl.pallas_call(
        functools.partial(widen_kernel, with_gram),
        in_specs=[IN_SMEM, IN_VMEM, IN_VMEM, IN_VMEM],
        out_specs=IN_VMEM,
        out_shape=jax.ShapeDtypeStruct(
            (columns // 2 + (RANK if with_gram else 0), RANK), jnp.float32
        ),
        scratch_shapes=[pltpu.VMEM((2 * RANK, rows), jnp.bfloat16)],
        cost_estimate=cost(4 * rows * columns * RANK),
        compiler_params=limit(16),
        name="widen_given" if with_gram else "widen_kept",
    )(core, momentum, gradient, projected)


def split_dot(left, right, dims):
    (a, b), (c, d) = left, right
    return mxu(a, c, dims) + (mxu(a, d, dims) + mxu(b, c, dims))


def limit(mib):
    return pltpu.CompilerParams(vmem_limit_bytes=mib << 20)


def folded(block):
    half = block.shape[0] // 2
    return jnp.concatenate((block[:half], block[half:]), axis=1)


def unfolded(block):
    return jnp.concatenate((block[:, :HALF], block[:, HALF:]), axis=0)


def merge_kernel(core, outgoing, received, kept, out):
    sides = out.shape[0]
    each = kept.shape[0] // sides
    for side in range(sides):
        span = pl.ds(side * each, each)
        out[side, :each, :] = kept[span, :] + received[span, :]
    gram = outgoing[kept.shape[0] :, :] + received[kept.shape[0] :, :]
    corner = gram[HALF:, :HALF]

    def put(square, strip):
        for side in range(sides):
            out[side, each : each + HALF // 2, :] = folded(square)
            out[side, each + HALF // 2 :, :] = folded(strip)

    @pl.when(core[0] == 0)
    def _():
        put(gram[:HALF, :HALF], corner[: HALF // 2])

    @pl.when(core[0] == 1)
    def _():
        put(gram[HALF:, HALF:], corner[HALF // 2 :])


def merge(core, outgoing, received, kept, sides):
    each = kept.shape[0] // sides
    return pl.pallas_call(
        merge_kernel,
        in_specs=[IN_SMEM, IN_VMEM, IN_VMEM, IN_VMEM],
        out_specs=IN_VMEM,
        out_shape=jax.ShapeDtypeStruct((sides, each + PACKED, RANK), jnp.float32),
        cost_estimate=cost(kept.size),
        compiler_params=pltpu.CompilerParams(vmem_limit_bytes=8 << 20),
        name="merge",
    )(core, outgoing, received, kept)


def summed_kernel(arrived, wide_out, gram_half):
    sides, each = arrived.shape[0], wide_out.shape[0]
    wide = arrived[0, :each, :]
    gram = arrived[0, each:, :]
    for side in range(1, sides):
        wide = wide + arrived[side, :each, :]
        gram = gram + arrived[side, each:, :]
    wide_out[...] = wide
    gram_half[...] = gram


def summed_over_sides(arrived):
    return pl.pallas_call(
        summed_kernel,
        in_specs=[IN_VMEM],
        out_specs=[IN_VMEM, IN_VMEM],
        out_shape=[
            jax.ShapeDtypeStruct((arrived.shape[1] - PACKED, RANK), jnp.float32),
            jax.ShapeDtypeStruct((PACKED, RANK), jnp.float32),
        ],
        cost_estimate=cost(arrived.size),
        compiler_params=limit(6),
        name="summed",
    )(arrived)


def inverse_factor(core, own, other, projected, out_ref, orthonormal, work):
    first = jnp.where(core[0] == 0, own[...], other[...])
    second = jnp.where(core[0] == 0, other[...], own[...])
    corner = jnp.concatenate((unfolded(first[HALF // 2 :]), unfolded(second[HALF // 2 :])), axis=0)
    gram = jnp.concatenate(
        (
            jnp.concatenate((unfolded(first[: HALF // 2]), corner.T), axis=1),
            jnp.concatenate((corner, unfolded(second[: HALF // 2])), axis=1),
        ),
        axis=0,
    )
    shape = (RANK, RANK)
    row, column = (lax.broadcasted_iota(jnp.int32, shape, d) for d in (0, 1))
    eye = (row == column).astype(jnp.float32)
    lower = jnp.where(row > column, 1.0, 0.5 * eye)
    diagonal = gram * eye
    along = lax.rsqrt(jnp.sum(diagonal, axis=0, keepdims=True))
    down = lax.rsqrt(jnp.sum(diagonal, axis=1, keepdims=True))
    scaled = gram * down * along

    def step(guess, dot):
        error = dot(dot(guess, scaled, PLAIN), guess, FLIPPED) - eye
        return guess - dot1(error * lower, guess, PLAIN), error

    guess = eye - (scaled - eye) * lower
    guess, _ = step(guess, dot1)
    guess, _ = step(guess, dot3)
    guess, error = step(guess, dot3)
    out_ref[...] = guess * along

    @pl.when(jnp.logical_not(jnp.sum(error * error) < 1e-4))
    def _():
        work[:, :RANK] = gram
        work[:, RANK:] = eye
        rows = lax.broadcasted_iota(jnp.int32, (RANK, 1), 0)
        lanes = lax.broadcasted_iota(jnp.int32, (1, RANK), 1)

        def eliminate(i, carry):
            line = work[pl.ds(i, 1), :]
            pivot = jnp.sum(jnp.where(lanes == i, line[:, :RANK], 0.0), axis=1, keepdims=True)
            root = lax.rsqrt(pivot)
            line = line * root
            whole = work[...]
            beneath = jnp.sum(jnp.where(lanes == i, whole[:, :RANK], 0.0), axis=1, keepdims=True) * root
            rest = whole - jnp.where(rows > i, beneath, 0.0) * line
            work[...] = jnp.where(rows == i, line, rest)
            return carry

        lax.fori_loop(0, RANK, eliminate, 0)
        out_ref[...] = jnp.where(row >= column, work[:, RANK:], 0.0)

    right = parts(out_ref[...])

    @pl.loop(0, projected.shape[0] // TILE)
    def _(t):
        span = pl.ds(pl.multiple_of(t * TILE, TILE), TILE)
        orthonormal[span, :] = split_dot(parts(projected[span, :]), right, FLIPPED)


def inverted(core, own, other, projected):
    return pl.pallas_call(
        inverse_factor,
        in_specs=[IN_SMEM, IN_VMEM, IN_VMEM, IN_VMEM],
        out_specs=[IN_VMEM, IN_VMEM],
        out_shape=[
            jax.ShapeDtypeStruct((RANK, RANK), jnp.float32),
            jax.ShapeDtypeStruct(projected.shape, jnp.float32),
        ],
        scratch_shapes=[pltpu.VMEM((RANK, 2 * RANK), jnp.float32)],
        cost_estimate=cost(1 << 32),
        compiler_params=limit(12),
        name="inverse_factor",
    )(core, own, other, projected)


def transposed_kernel(line, *refs):
    *pieces, inverse, out, squares = refs
    right = parts(inverse[...])
    total = jnp.zeros((1, RANK), jnp.float32)
    for k, piece in enumerate(pieces):
        tile = split_dot(parts(piece[...]), right, FLIPPED)
        start = lax.rem(line[0] + len(pieces) - k, len(pieces)) * piece.shape[0]
        out[pl.ds(pl.multiple_of(start, HALF), piece.shape[0]), :] = tile
        total += jnp.sum(tile * tile, axis=0, keepdims=True)
    squares[...] = jnp.broadcast_to(total[None], squares.shape)


def transpose_of(line, pieces, inverse, copies):
    rows = len(pieces) * pieces[0].shape[0]
    return pl.pallas_call(
        transposed_kernel,
        in_specs=[IN_SMEM] + [IN_VMEM] * (len(pieces) + 1),
        out_specs=[IN_VMEM, IN_VMEM],
        out_shape=[
            jax.ShapeDtypeStruct((rows, RANK), jnp.float32),
            jax.ShapeDtypeStruct((copies, 1, RANK), jnp.float32),
        ],
        cost_estimate=cost(6 * rows * RANK * RANK),
        compiler_params=limit(8),
        name="transposed",
    )(line, *pieces, inverse)


SPAN = 512


def momentum_kernel(core, momentum, gradient, orthonormal, own, other, out, top, low):
    @pl.when(pl.program_id(1) == 0)
    def _():
        top[...], low[...] = parts(jnp.where(pl.program_id(0) == 0, own[...], other[...]))

    left = parts((1.0 - momentum_decay) * orthonormal[...])
    product = split_dot(left, (top[...], low[...]), FLIPPED)
    out[...] = (wider(momentum[...]) + wider(gradient[...]) - product).astype(jnp.bfloat16)


def side_of(h, core):
    return h + core[0] - 2 * h * core[0]


def remembered(core, momentum, gradient, orthonormal, own, other):
    rows, half = orthonormal.shape[0], own.shape[0]
    block = pl.BlockSpec((SPAN, half), lambda h, t, core: (t, side_of(h, core)))
    whole = pl.BlockSpec((half, RANK), lambda h, t, core: (0, 0))
    return pl.pallas_call(
        momentum_kernel,
        grid_spec=pltpu.PrefetchScalarGridSpec(
            num_scalar_prefetch=1,
            grid=(2, rows // SPAN),
            in_specs=[
                block,
                block,
                pl.BlockSpec((SPAN, RANK), lambda h, t, core: (t, 0)),
                whole,
                whole,
            ],
            out_specs=block,
            scratch_shapes=[pltpu.VMEM((half, RANK), jnp.bfloat16)] * 2,
        ),
        out_shape=jax.ShapeDtypeStruct((rows, 2 * half), jnp.bfloat16),
        cost_estimate=cost(1 << 32),
        compiler_params=pltpu.CompilerParams(vmem_limit_bytes=20 << 20),
        name="new_momentum",
    )(core, *in_hbm(momentum, gradient), orthonormal, own, other)


def update_kernel(core, orthonormal, own, other, squares, update, basis, top, low):
    norms = jnp.sqrt(jnp.sum(squares[...], axis=0)) + eps

    @pl.when(pl.program_id(1) == 0)
    def _():
        side = jnp.where(pl.program_id(0) == 0, own[...], other[...])
        top[...], low[...] = parts(side)
        basis[...] = side / norms

    left = parts(orthonormal[...] * (math.sqrt(ROWS * COLS / RANK) / norms))
    update[...] = split_dot(left, (top[...], low[...]), FLIPPED)


def updated(core, orthonormal, own, other, squares):
    rows, half = orthonormal.shape[0], own.shape[0]
    whole = pl.BlockSpec((half, RANK), lambda h, t, core: (0, 0))
    return pl.pallas_call(
        update_kernel,
        grid_spec=pltpu.PrefetchScalarGridSpec(
            num_scalar_prefetch=1,
            grid=(2, 1),
            in_specs=[
                pl.BlockSpec((rows, RANK), lambda h, t, core: (t, 0)),
                whole,
                whole,
                pl.BlockSpec(squares.shape, lambda h, t, core: (0, 0, 0)),
            ],
            out_specs=[
                pl.BlockSpec((rows, half), lambda h, t, core: (t, side_of(h, core))),
                pl.BlockSpec((half, RANK), lambda h, t, core: (side_of(h, core), 0)),
            ],
            scratch_shapes=[pltpu.VMEM((half, RANK), jnp.bfloat16)] * 2,
        ),
        out_shape=[
            jax.ShapeDtypeStruct((rows, 2 * half), jnp.float32),
            jax.ShapeDtypeStruct((2 * half, RANK), jnp.float32),
        ],
        cost_estimate=cost(6 * rows * 2 * half * RANK),
        compiler_params=limit(20),
        name="update",
    )(core, orthonormal, own, other, squares)


def step(momentum, gradient, right_basis):
    core, line = place_on("c"), place_on("x")
    sides = lax.axis_size("x")

    part = project(momentum, gradient, right_basis)
    part, core, line = lax.optimization_barrier((part, core, line))
    own = scattered(scattered(part, "y"), "z")
    projected = gathered(gathered(own, "z"), "y")

    outgoing = widen(True, core, momentum, gradient, projected)
    received = other_core(outgoing)
    kept = widen(False, core, momentum, gradient, projected)
    tiles = merge(core, outgoing, received, kept, sides)
    wide, gram_half = summed_over_sides(lax.all_to_all(tiles, "x", 0, 0, tiled=True))
    pieces = from_others(wide, "x")
    inverse, orthonormal = inverted(core, gram_half, other_core(gram_half), projected)

    everyone = ("c", *COL)
    own, squares = transpose_of(line, pieces, inverse, lax.axis_size(everyone))
    squares = lax.all_to_all(squares, everyone, 0, 0, tiled=True)
    other = other_core(own)
    new_momentum = remembered(core, momentum, gradient, orthonormal, own, other)
    update, new_basis = updated(core, orthonormal, own, other, squares)
    return (new_momentum, new_basis, update)


def solution(mesh):
    split = Mesh(mesh.devices.reshape(4, 2, 8, 4), (*ROW, *COL))
    placed = (P(ROW, COL), P(ROW, COL), P(COL, None))
    return jax.shard_map(
        step,
        mesh=split,
        in_specs=placed,
        out_specs=(P(ROW, COL), P(COL, None), P(ROW, COL)),
        check_vma=False,
    )
```
